32 devices in a mesh: mem: 2 (over x), col: 16 (over z, y, core).
Axes of the slice: x: 2, y: 2, z: 4, core: 2. Of those that a mesh axis runs over, the one named last changes fastest.
Arguments:
- state_a: bfloat16 [64, 1048576], P('mem', 'col'), may hold values from -12 to 12
- state_b: bfloat16 [64, 1048576], P('mem', 'col'), may hold values from -12 to 12
- obs_index: int32 [2, 8192, 16], P(None, ('col', 'mem')), may hold values from 0 to 127
- observation_count: int32 [2, 8192], P(None, ('col', 'mem')), may hold values from 1 to 16, as said below
- obs_value: float32 [2, 8192, 16], P(None, ('col', 'mem')), may hold values from -32 to 32
- obs_weight: float32 [2, 8192, 16], P(None, ('col', 'mem')), may hold values from 0.02 to 0.2
Outputs:
- analysis_a: bfloat16 [64, 1048576], P(None, ('col', 'mem'))
- analysis_b: bfloat16 [64, 1048576], P(None, ('col', 'mem'))
- transform: float32 [64, 64], replicated
The draws below stay inside these ranges and needn't reach their ends.
Inputs may be any that keep to these rules, and one draw needn't show every extreme that they name: Slot s of block b of group g is an observation when s < observation_count[g, b]; for each group, every aligned run of 256 blocks holds a block with all 16 slots live.
All inputs are finite; a program needn't handle non-finite values.
Results may differ from the reference program's by a relative error of at most 0.005.
Values may be sent and summed in bfloat16 or wider, within the bound.
No kernel may reach another device: no remote copies, remote signals or barrier semaphores. Data moves between devices by JAX's collectives and lax.ppermute only.
A program may use at most 64 MiB of HBM per device.

```python
import math
import jax
import jax.numpy as jnp
from jax import lax

K = 64
OBS_BLK = 16
ITERS = 24
NCOL = 1048576
PIECE = 32768
BPD = 256
NBLK = 8192


def group_parts(key, salt):
    key = jax.random.fold_in(key, salt)
    subkeys = jax.random.split(key, 8)
    patterns = jax.random.normal(subkeys[0], (K, 3), jnp.float32)
    amplitudes = jnp.exp(jax.random.uniform(subkeys[1], (3, 16), jnp.float32, jnp.log(0.2), jnp.log(1.6)))
    coefficients = jax.random.normal(subkeys[2], (3, NCOL), jnp.float32)
    scales = jnp.exp(jax.random.uniform(subkeys[3], (K,), jnp.float32, jnp.log(0.5), jnp.log(2.0)))
    member_noise = 0.5 * jax.random.normal(subkeys[4], (K, NCOL), jnp.float32)
    truth_noise = 0.5 * jax.random.normal(subkeys[5], (NCOL,), jnp.float32)
    offsets = jax.random.uniform(subkeys[6], (3,), jnp.float32, 1.0, 2.0)
    sign_flip = jnp.where(jax.random.uniform(subkeys[7], (3,), jnp.float32) < 0.5, -1.0, 1.0)
    driving = jnp.repeat(amplitudes, NCOL // 16, axis=1) * coefficients
    truth_coef = jnp.mean(patterns, axis=0) + offsets * sign_flip
    return (patterns, driving, scales, member_noise, truth_noise, truth_coef)


def member_field(key, salt):
    patterns, driving, scales, member_noise, truth_noise, truth_coef = group_parts(key, salt)
    member_values = scales[:, None] * member_noise + jnp.dot(patterns, driving, precision=lax.Precision.HIGHEST)
    return jnp.clip(member_values, -12.0, 12.0).astype(jnp.bfloat16)


def index_table(key):
    return jax.random.randint(jax.random.fold_in(key, 41), (2, NBLK, OBS_BLK), 0, 128).astype(jnp.int32)


def draw_state_a(key, part):
    return member_field(key, 11)


def draw_state_b(key, part):
    return member_field(key, 23)


def draw_obs_index(key, part):
    return index_table(key)


def draw_obs_value(key, part):
    observation_lookup = index_table(key)
    picked = []
    for group, salt in enumerate((11, 23)):
        patterns, driving, scales, member_noise, truth_noise, truth_coef = group_parts(key, salt)
        truth_field = jnp.dot(truth_coef, driving, precision=lax.Precision.HIGHEST) + truth_noise
        truth_field = jnp.clip(truth_field, -12.0, 12.0)
        picked.append(jnp.take_along_axis(truth_field.reshape(NBLK, 128), observation_lookup[group], axis=1))
    error_key = jax.random.fold_in(key, 53)
    errors = jnp.clip(jax.random.normal(error_key, (2, NBLK, OBS_BLK), jnp.float32), -4.0, 4.0)
    return jnp.stack(picked) + 5.0 * errors


def draw_observation_count(key, part):
    key = jax.random.fold_in(key, 37)
    first, second = jax.random.split(key)
    segs = NBLK // BPD
    counts = jax.random.randint(first, (2, segs, BPD), 1, OBS_BLK + 1)
    where_full = jax.random.randint(second, (2, segs, 1), 0, BPD)
    position = lax.broadcasted_iota(jnp.int32, (2, segs, BPD), 2)
    counts = jnp.where(position == where_full, OBS_BLK, counts)
    return counts.reshape(2, NBLK).astype(jnp.int32)


def level_of(stream_key, shape, cuts, low, top_value):
    def one(axis_at, blocks):
        heights = jax.random.uniform(jax.random.fold_in(jax.random.fold_in(stream_key, 6), axis_at), (blocks,), jnp.float32, low / len(cuts), top_value / len(cuts))
        return jnp.repeat(jnp.exp(heights), shape[axis_at] // blocks).reshape((-1,) + (1,) * (len(shape) - axis_at - 1))

    loudness = one(*cuts[0])
    for cut in cuts[1:]:
        loudness = loudness * one(*cut)
    return loudness


def setup_inputs(seed: int = 0) -> dict:
    splits = jax.random.split(jax.random.key(seed), 7)
    return {
        "state_a": draw_state_a(jax.random.fold_in(splits[6], 71), 0),
        "state_b": draw_state_b(jax.random.fold_in(splits[6], 71), 0),
        "obs_index": draw_obs_index(jax.random.fold_in(splits[6], 71), 0),
        "observation_count": draw_observation_count(jax.random.fold_in(splits[6], 71), 0),
        "obs_value": draw_obs_value(jax.random.fold_in(splits[6], 71), 0),
        "obs_weight": jnp.clip(jnp.exp(math.log(0.2) - 2.3025851 * jax.random.uniform(splits[5], (2, NBLK, OBS_BLK), jnp.float32) ** level_of(splits[5], (2, NBLK, OBS_BLK), ((1, 32),), -0.2, 0.2)), 0.02, 0.2),
    }


def inverse_root(amat):
    scale = jnp.sqrt(jnp.sum(amat * amat))
    eye = jnp.eye(amat.shape[0], dtype=jnp.float32)

    def forward_step(step, carry):
        yn, zn = carry
        tm = 1.5 * eye - 0.5 * jnp.dot(zn, yn, precision=lax.Precision.HIGHEST)
        return (jnp.dot(yn, tm, precision=lax.Precision.HIGHEST), jnp.dot(tm, zn, precision=lax.Precision.HIGHEST))
    yn, zn = lax.fori_loop(0, ITERS, forward_step, (amat / scale, eye))
    return (zn, scale)

def make_transform(gram_product, cross, misfit, total):
    members = gram_product.shape[0]
    scl = (members - 1.0) / total
    gs = scl * gram_product
    bs = scl * cross
    qval = scl * misfit
    tval = jnp.trace(gs)
    rho = (1.0 + qval / (members - 1.0)) / (1.0 + tval / (members - 1.0))
    amat = (members - 1.0) / rho * jnp.eye(members, dtype=jnp.float32) + gs
    zn, scale = inverse_root(amat)
    pmat = jnp.dot(zn, zn, precision=lax.Precision.HIGHEST) / scale
    wbar = jnp.dot(pmat, bs, precision=lax.Precision.HIGHEST)
    return jnp.sqrt(members - 1.0) * zn / jnp.sqrt(scale) + wbar[:, None]

def reference(state_a, state_b, obs_index, observation_count, obs_value, obs_weight):
    segs = NCOL // PIECE
    states = (state_a, state_b)

    def accumulate(carry, seg):
        gram_product, cross, misfit, total = carry
        for group in range(2):
            cols = lax.dynamic_slice_in_dim(states[group], seg * PIECE, PIECE, 1)
            idx = lax.dynamic_slice_in_dim(obs_index[group], seg * BPD, BPD, 0)
            cnt = lax.dynamic_slice_in_dim(observation_count[group], seg * BPD, BPD, 0)
            val = lax.dynamic_slice_in_dim(obs_value[group], seg * BPD, BPD, 0)
            wgt = lax.dynamic_slice_in_dim(obs_weight[group], seg * BPD, BPD, 0)
            live = (lax.broadcasted_iota(jnp.int32, (BPD, OBS_BLK), 1) < cnt[:, None]).astype(jnp.float32)
            blocks = cols.reshape(K, BPD, 128)
            hx = jnp.take_along_axis(blocks, jnp.broadcast_to(idx[None], (K, BPD, OBS_BLK)), axis=2).astype(jnp.float32)
            hmean = lax.optimization_barrier(jnp.mean(hx, axis=0))
            anomaly_rows = hx - hmean[None]
            innov = val - hmean
            wt = live * wgt
            scaled_anomaly = anomaly_rows * wt[None]
            gram_product = gram_product + jnp.einsum('nix,fix->nf', scaled_anomaly, anomaly_rows, precision=lax.Precision.HIGHEST)
            cross = cross + jnp.einsum('kbs,bs->k', scaled_anomaly, innov, precision=lax.Precision.HIGHEST)
            misfit = misfit + jnp.sum(wt * innov * innov)
            total = total + jnp.sum(live)
        return ((gram_product, cross, misfit, total), None)
    init = (jnp.zeros((K, K), jnp.float32), jnp.zeros((K,), jnp.float32), jnp.zeros((), jnp.float32), jnp.zeros((), jnp.float32))
    (gram_product, cross, misfit, total), _ = lax.scan(accumulate, init, jnp.arange(segs, dtype=jnp.int32))
    transform = make_transform(gram_product, cross, misfit, total)
    wb = transform.astype(jnp.bfloat16)
    column_total = lax.optimization_barrier(jnp.sum(wb.astype(jnp.float32), axis=0))
    ones = jnp.ones((K,), jnp.bfloat16)

    def analyse(state):

        def one_seg(seg):
            cols = lax.dynamic_slice_in_dim(state, seg * PIECE, PIECE, 1)
            xmean = jnp.dot(ones, cols, preferred_element_type=jnp.float32) / K
            mixed = jnp.dot(wb.T, cols, preferred_element_type=jnp.float32)
            return (mixed + xmean[None, :] * (1.0 - column_total)[:, None]).astype(jnp.bfloat16)
        pieces = lax.map(one_seg, jnp.arange(segs, dtype=jnp.int32))
        return jnp.transpose(pieces, (1, 0, 2)).reshape(K, NCOL)
    return (analyse(state_a), analyse(state_b), transform)
```

```python
import functools

import jax
import jax.numpy as jnp
from jax import lax
from jax.experimental import pallas as pl
from jax.experimental.pallas import tpu as pltpu
from jax.sharding import PartitionSpec as P


ITERS = 24
LANES = 128

MESSAGES = (
    (0, 0, 1),
    (0, 1, 3),
    (0, 3, 5),
    (0, 5, 8),
    (1, 0, 4),
    (1, 4, 6),
    (1, 6, 7),
    (1, 7, 8),
)


def split(x):
    high = x.astype(jnp.bfloat16)
    rest = x - high.astype(jnp.float32)
    middle = rest.astype(jnp.bfloat16)
    return high, middle, (rest - middle.astype(jnp.float32)).astype(jnp.bfloat16)


def terms_dot(a, b):
    rows = a[0].shape[0]
    stacked = jnp.concatenate(a, axis=0)
    by_high = jnp.dot(stacked, b[0], preferred_element_type=jnp.float32)
    by_middle = jnp.dot(stacked[: 2 * rows], b[1], preferred_element_type=jnp.float32)
    by_low = jnp.dot(a[0], b[2], preferred_element_type=jnp.float32)
    second = by_high[rows : 2 * rows] + by_middle[:rows]
    third = by_high[2 * rows :] + by_middle[rows:] + by_low
    return by_high[:rows] + (second + third)


def gather_kernel(slots, base_ref, index_ref, a_ref, b_ref, out_ref):
    per = LANES // slots
    step = pl.program_id(0)
    width = out_ref.shape[2]
    rows = a_ref.shape[0]
    place = lax.broadcasted_iota(jnp.int32, (rows, LANES), 1) // slots
    for group, ref in enumerate((a_ref, b_ref)):
        for q in range(width // LANES):
            row = index_ref[group, pl.ds(step * (width // LANES) + q, 1), :]
            wanted = jnp.broadcast_to(row, (rows, LANES))
            acc = jnp.zeros((rows, LANES), jnp.float32)
            for j in range(per):
                start = (q * per + j) * LANES
                block = ref[:, start : start + LANES].astype(jnp.float32)
                taken = jnp.take_along_axis(block, wanted, axis=1, mode="promise_in_bounds")
                acc = jnp.where(place == j, taken, acc)
            out_ref[group, :, q * LANES : (q + 1) * LANES] = acc.astype(out_ref.dtype)


def gather(state_a, state_b, index, base, slots, piece):
    rows = state_a.shape[0]
    width = min(4096, piece)
    steps = piece // width
    observations = piece // LANES * slots
    state_spec = pl.BlockSpec((rows, width), lambda i, base: (0, base[0] * steps + i))
    return pl.pallas_call(
        functools.partial(gather_kernel, slots),
        out_shape=jax.ShapeDtypeStruct((2, rows, observations), jnp.bfloat16),
        grid_spec=pltpu.PrefetchScalarGridSpec(
            num_scalar_prefetch=1,
            grid=(steps,),
            in_specs=[
                pl.BlockSpec(index.shape, lambda i, base: (0, 0, 0)),
                state_spec,
                state_spec,
            ],
            out_specs=pl.BlockSpec((2, rows, observations // steps), lambda i, base: (0, 0, i)),
        ),
        compiler_params=pltpu.CompilerParams(dimension_semantics=("arbitrary",)),
        name="gather",
    )(base, index, state_a, state_b)


def stats_kernel(parts, me_ref, *refs):
    hx_refs = refs[:parts]
    value_ref, weight_ref, live_ref, out_ref, all_ref = refs[parts:]
    members = hx_refs[0].shape[1]
    everyone = members * parts
    me = me_ref[0]
    for j in range(parts):
        at = pl.multiple_of(lax.rem(me + j, parts) * members, members)
        all_ref[pl.ds(at, members), :] = hx_refs[j][0].astype(jnp.float32)
    hx = all_ref[...]
    hmean = jnp.sum(hx, axis=0, keepdims=True) / everyone
    anomaly = hx - hmean
    innov = value_ref[0] - hmean
    wt = weight_ref[0]
    scaled = anomaly * wt
    product = lax.dot_general(
        jnp.concatenate(split(scaled), axis=0),
        jnp.concatenate(split(anomaly), axis=0),
        (((1,), (1,)), ((), ())),
        preferred_element_type=jnp.float32,
    )

    def term(i, j):
        rows = product[i * everyone : (i + 1) * everyone]
        return rows[:, j * everyone : (j + 1) * everyone]

    gram = term(0, 0) + (term(0, 1) + term(1, 0) + (term(0, 2) + term(2, 0) + term(1, 1)))
    cross = jnp.sum(scaled * innov, axis=1, keepdims=True)
    misfit = jnp.sum(wt * innov * innov, axis=1, keepdims=True)
    total = jnp.sum(live_ref[0], axis=1, keepdims=True)
    lane = lax.broadcasted_iota(jnp.int32, (everyone, LANES - everyone), 1)
    side = jnp.where(lane == 0, cross, jnp.where(lane == 1, misfit, jnp.where(lane == 2, total, 0.0)))
    new = jnp.concatenate([gram, side], axis=1)
    first = (pl.program_id(0) == 0) & (pl.program_id(1) == 0)

    @pl.when(first)
    def _():
        out_ref[...] = new

    @pl.when(jnp.logical_not(first))
    def _():
        out_ref[...] += new


def statistics(parts, value, weight, live, me):
    members, observations = parts[0].shape[1:]
    everyone = members * len(parts)
    width = min(1024, observations)
    hx_spec = pl.BlockSpec((1, members, width), lambda g, i, me: (g, 0, i))
    row_spec = pl.BlockSpec((1, 1, width), lambda g, i, me: (g, 0, i))
    return pl.pallas_call(
        functools.partial(stats_kernel, len(parts)),
        out_shape=jax.ShapeDtypeStruct((everyone, LANES), jnp.float32),
        grid_spec=pltpu.PrefetchScalarGridSpec(
            num_scalar_prefetch=1,
            grid=(2, observations // width),
            in_specs=[hx_spec] * len(parts) + [row_spec] * 3,
            out_specs=pl.BlockSpec((everyone, LANES), lambda g, i, me: (0, 0)),
            scratch_shapes=[pltpu.VMEM((everyone, width), jnp.float32)],
        ),
        compiler_params=pltpu.CompilerParams(dimension_semantics=("arbitrary", "arbitrary")),
        name="statistics",
    )(me, *parts, value, weight, live)


def transform_kernel(members, me_ref, stats_ref, transform_ref, mixer_ref, rest_ref):
    stats = stats_ref[...]
    everyone = stats.shape[0]
    gram = stats[:, :everyone]
    cross = stats[:, everyone : everyone + 1]
    misfit = stats[0:1, everyone + 1 : everyone + 2]
    total = stats[0:1, everyone + 2 : everyone + 3]
    dof = everyone - 1.0
    row = lax.broadcasted_iota(jnp.int32, (everyone, everyone), 0)
    col = lax.broadcasted_iota(jnp.int32, (everyone, everyone), 1)
    eye = (row == col).astype(jnp.float32)
    scl = dof / total
    gs = scl * gram
    bs = scl * cross
    qval = scl * misfit

    def whole_sum(x):
        return jnp.sum(jnp.sum(x, axis=1, keepdims=True), axis=0, keepdims=True)

    tval = whole_sum(gs * eye)
    rho = (1.0 + qval / dof) / (1.0 + tval / dof)
    amat = dof / rho * eye + gs
    scale = jnp.sqrt(whole_sum(amat * amat))

    def forward_step(_, carry):
        yn, zn = (split(x) for x in carry)
        tm = split(1.5 * eye - 0.5 * terms_dot(zn, yn))
        return terms_dot(yn, tm), terms_dot(tm, zn)

    _, zn = lax.fori_loop(0, ITERS, forward_step, (amat / scale, eye))
    parts = split(zn)
    pmat = terms_dot(parts, parts) / scale
    wide = jnp.broadcast_to(bs, (everyone, LANES))
    wbar = terms_dot(split(pmat), split(wide))[:, 0:1]
    transform = jnp.sqrt(dof) * zn / jnp.sqrt(scale) + wbar
    transform_ref[...] = transform
    held = pltpu.roll(transform, lax.rem(everyone - me_ref[0] * members, everyone), 0)
    mixer = held.T.astype(jnp.bfloat16)
    column_total = jnp.sum(mixer.astype(jnp.float32), axis=1, keepdims=True)
    extra = mixer_ref.shape[0] - everyone
    mixer_ref[...] = jnp.concatenate([mixer, jnp.ones((extra, everyone), jnp.bfloat16)], axis=0)
    rest_ref[...] = jnp.broadcast_to((1.0 - column_total) / everyone, rest_ref.shape)


def make_transform(stats, members, me):
    everyone = stats.shape[0]
    return pl.pallas_call(
        functools.partial(transform_kernel, members),
        out_shape=(
            jax.ShapeDtypeStruct((everyone, everyone), jnp.float32),
            jax.ShapeDtypeStruct((everyone + 16, everyone), jnp.bfloat16),
            jax.ShapeDtypeStruct((everyone, LANES), jnp.float32),
        ),
        in_specs=[pl.BlockSpec(memory_space=pltpu.SMEM), pl.BlockSpec(memory_space=pltpu.VMEM)],
        out_specs=(pl.BlockSpec(memory_space=pltpu.VMEM),) * 3,
        name="transform",
    )(me, stats)


def analysis_kernel(parts, aliased, base_ref, mixer_ref, rest_ref, *refs):
    cols_refs = refs[:parts]
    out_ref = refs[parts + aliased]
    everyone = out_ref.shape[0]
    members = cols_refs[0].shape[0]
    if members % 16 == 0:
        cols = jnp.concatenate([ref[...] for ref in cols_refs], axis=0)
        mixed = jnp.dot(mixer_ref[...], cols, preferred_element_type=jnp.float32)
    else:
        cols = jnp.concatenate([ref[...].astype(jnp.float32) for ref in cols_refs], axis=0)
        mixed = jnp.dot(
            mixer_ref[...], cols.astype(jnp.bfloat16), preferred_element_type=jnp.float32
        )
    rest = rest_ref[:, 0:1]
    out = mixed[:everyone] + rest * mixed[everyone : everyone + 1]
    out_ref[...] = out.astype(out_ref.dtype)


def analyse(out, state, received, mixer, rest, base, first, piece):
    members, length = received[0].shape
    everyone = rest.shape[0]
    width = min(2048, length)
    steps = length // width
    skip = first // width
    whole = piece // width
    parts = len(received) + 1
    aliased = int(out is not None)
    in_specs = [
        pl.BlockSpec(mixer.shape, lambda i, base: (0, 0)),
        pl.BlockSpec(rest.shape, lambda i, base: (0, 0)),
        pl.BlockSpec((members, width), lambda i, base: (0, base[0] * whole + skip + i)),
    ] + [pl.BlockSpec((members, width), lambda i, base: (0, i))] * len(received)
    operands = [base, mixer, rest, state, *received]
    aliases = {}
    if aliased:
        in_specs.append(pl.BlockSpec(memory_space=pl.ANY))
        aliases = {len(operands): 0}
        operands.append(out)
    return pl.pallas_call(
        functools.partial(analysis_kernel, parts, aliased),
        out_shape=jax.ShapeDtypeStruct((everyone, piece), jnp.bfloat16),
        grid_spec=pltpu.PrefetchScalarGridSpec(
            num_scalar_prefetch=1,
            grid=(steps,),
            in_specs=in_specs,
            out_specs=pl.BlockSpec((everyone, width), lambda i, base: (0, skip + i)),
        ),
        input_output_aliases=aliases,
        compiler_params=pltpu.CompilerParams(dimension_semantics=("arbitrary",)),
        name="analysis",
    )(*operands)


def shards(state_a, state_b, obs_index, observation_count, obs_value, obs_weight):
    states = (state_a, state_b)
    members = state_a.shape[0]
    nmem = lax.axis_size("mem")
    ncol = lax.axis_size("col")
    piece = state_a.shape[1] // nmem
    nblk = obs_index.shape[1]
    slots = obs_index.shape[2]
    observations = nblk * slots
    unit = piece // 8
    me = lax.axis_index("mem")
    me_ref = me[None].astype(jnp.int32)
    shifts = range(1, nmem)

    def to_lower(array, shift):
        return lax.ppermute(array, "mem", [(i, (i - shift) % nmem) for i in range(nmem)])

    def to_upper(array, shift):
        return lax.ppermute(array, "mem", [(i, (i + shift) % nmem) for i in range(nmem)])

    def cut(message, source):
        group, lo, hi = message
        return [
            lax.dynamic_slice(
                source[group],
                (0, lax.rem(me + nmem - shift, nmem) * piece + lo * unit),
                (members, (hi - lo) * unit),
            )
            for shift in shifts
        ]

    index = obs_index.reshape(2, observations // LANES, LANES)
    others_index = [to_upper(index, shift) for shift in shifts]

    own_hx = gather(state_a, state_b, index, me_ref, slots, piece)
    sent_hx = [
        gather(state_a, state_b, idx, lax.rem(me_ref + nmem - shift, nmem), slots, piece)
        for idx, shift in zip(others_index, shifts)
    ]
    got_hx = [to_lower(x, shift) for x, shift in zip(sent_hx, shifts)]

    live = (
        lax.broadcasted_iota(jnp.int32, (2, nblk, slots), 2) < observation_count[:, :, None]
    ).astype(jnp.float32)
    weight = (live * obs_weight).reshape(2, 1, observations)
    live = live.reshape(2, 1, observations)
    value = obs_value.reshape(2, 1, observations)
    stats = statistics([own_hx, *got_hx], value, weight, live, me_ref)

    received = []
    for i, message in enumerate(MESSAGES):
        if i < len(MESSAGES) - 1:
            pieces = cut(message, states)
        else:
            pieces = cut(message, lax.optimization_barrier((*states, stats)))
        received.append([to_lower(x, shift) for x, shift in zip(pieces, shifts)])

    def all_sum(x, axis, size):
        step = 1
        while step < size:
            x = x + lax.ppermute(x, axis, [(i, i ^ step) for i in range(size)])
            step *= 2
        return x

    stats = all_sum(all_sum(stats, "mem", nmem), "col", ncol)
    transform, mixer, rest = make_transform(stats, members, me_ref)

    outs = [None, None]
    for (group, lo, hi), pieces in zip(MESSAGES, received):
        outs[group] = analyse(
            outs[group], states[group], pieces, mixer, rest, me_ref, lo * unit, piece
        )
    return (outs[0], outs[1], transform)


def solution(mesh):
    return jax.shard_map(
        shards,
        mesh=mesh,
        in_specs=(
            P("mem", "col"),
            P("mem", "col"),
            P(None, ("col", "mem"), None),
            P(None, ("col", "mem")),
            P(None, ("col", "mem"), None),
            P(None, ("col", "mem"), None),
        ),
        out_specs=(P(None, ("col", "mem")), P(None, ("col", "mem")), P()),
        check_vma=False,
    )
```

```python
import functools
import math

import jax
import jax.numpy as jnp
from jax import lax
from jax.experimental import pallas as pl
from jax.experimental.pallas import tpu as pltpu
from jax.sharding import PartitionSpec as P


ITERS = 24
VMEM = 16 * 1024 * 1024
LANES = 128

MESSAGES = (
    (0, 0, 2),
    (0, 2, 4),
    (0, 4, 8),
    (1, 0, 4),
    (1, 4, 6),
    (1, 6, 8),
)
CALLS = ((0, 1, 2), (3,), (4,), (5,))


def split(x):
    high = x.astype(jnp.bfloat16)
    rest = x - high.astype(jnp.float32)
    middle = rest.astype(jnp.bfloat16)
    return high, middle, (rest - middle.astype(jnp.float32)).astype(jnp.bfloat16)


def terms_dot(a, b):
    rows = a[0].shape[0]
    stacked = jnp.concatenate(a, axis=0)
    by_high = jnp.dot(stacked, b[0], preferred_element_type=jnp.float32)
    by_middle = jnp.dot(stacked[: 2 * rows], b[1], preferred_element_type=jnp.float32)
    by_low = jnp.dot(a[0], b[2], preferred_element_type=jnp.float32)
    second = by_high[rows : 2 * rows] + by_middle[:rows]
    third = by_high[2 * rows :] + by_middle[rows:] + by_low
    return by_high[:rows] + (second + third)


def gather_kernel(slots, base_ref, index_ref, a_ref, b_ref, out_ref):
    per = LANES // slots
    step = pl.program_id(0)
    width = out_ref.shape[2]
    rows = a_ref.shape[0]
    place = lax.broadcasted_iota(jnp.int32, (rows, LANES), 1) // slots
    for group, ref in enumerate((a_ref, b_ref)):
        for q in range(width // LANES):
            row = index_ref[group, pl.ds(step * (width // LANES) + q, 1), :]
            wanted = jnp.broadcast_to(row, (rows, LANES))
            acc = jnp.zeros((rows, LANES), jnp.float32)
            for j in range(per):
                start = (q * per + j) * LANES
                block = ref[:, start : start + LANES].astype(jnp.float32)
                taken = jnp.take_along_axis(block, wanted, axis=1, mode="promise_in_bounds")
                acc = jnp.where(place == j, taken, acc)
            out_ref[group, :, q * LANES : (q + 1) * LANES] = acc.astype(out_ref.dtype)


def gather(state_a, state_b, index, base, slots, piece):
    rows = state_a.shape[0]
    width = min(4096, piece)
    steps = piece // width
    observations = piece // LANES * slots
    state_spec = pl.BlockSpec((rows, width), lambda i, base: (0, base[0] * steps + i))
    return pl.pallas_call(
        functools.partial(gather_kernel, slots),
        out_shape=jax.ShapeDtypeStruct((2, rows, observations), jnp.bfloat16),
        grid_spec=pltpu.PrefetchScalarGridSpec(
            num_scalar_prefetch=1,
            grid=(steps,),
            in_specs=[
                pl.BlockSpec(index.shape, lambda i, base: (0, 0, 0)),
                state_spec,
                state_spec,
            ],
            out_specs=pl.BlockSpec((2, rows, observations // steps), lambda i, base: (0, 0, i)),
        ),
        compiler_params=pltpu.CompilerParams(dimension_semantics=("arbitrary",)),
        name="gather",
    )(base, index, state_a, state_b)


def stats_kernel(parts, me_ref, *refs):
    hx_refs = refs[:parts]
    value_ref, weight_ref, live_ref, out_ref, all_ref = refs[parts:]
    members = hx_refs[0].shape[1]
    everyone = members * parts
    me = me_ref[0]
    for j in range(parts):
        at = pl.multiple_of(lax.rem(me + j, parts) * members, members)
        all_ref[pl.ds(at, members), :] = hx_refs[j][0].astype(jnp.float32)
    hx = all_ref[...]
    hmean = jnp.sum(hx, axis=0, keepdims=True) / everyone
    anomaly = hx - hmean
    innov = value_ref[0] - hmean
    wt = weight_ref[0]
    scaled = anomaly * wt
    product = lax.dot_general(
        jnp.concatenate(split(scaled), axis=0),
        jnp.concatenate(split(anomaly), axis=0),
        (((1,), (1,)), ((), ())),
        preferred_element_type=jnp.float32,
    )

    def term(i, j):
        rows = product[i * everyone : (i + 1) * everyone]
        return rows[:, j * everyone : (j + 1) * everyone]

    gram = term(0, 0) + (term(0, 1) + term(1, 0) + (term(0, 2) + term(2, 0) + term(1, 1)))
    cross = jnp.sum(scaled * innov, axis=1, keepdims=True)
    misfit = jnp.sum(wt * innov * innov, axis=1, keepdims=True)
    total = jnp.sum(live_ref[0], axis=1, keepdims=True)
    lane = lax.broadcasted_iota(jnp.int32, (everyone, LANES - everyone), 1)
    side = jnp.where(lane == 0, cross, jnp.where(lane == 1, misfit, jnp.where(lane == 2, total, 0.0)))
    new = jnp.concatenate([gram, side], axis=1)
    first = (pl.program_id(0) == 0) & (pl.program_id(1) == 0)

    @pl.when(first)
    def _():
        out_ref[...] = new

    @pl.when(jnp.logical_not(first))
    def _():
        out_ref[...] += new


def statistics(parts, value, weight, live, me):
    members, observations = parts[0].shape[1:]
    everyone = members * len(parts)
    width = min(1024, observations)
    hx_spec = pl.BlockSpec((1, members, width), lambda g, i, me: (g, 0, i))
    row_spec = pl.BlockSpec((1, 1, width), lambda g, i, me: (g, 0, i))
    return pl.pallas_call(
        functools.partial(stats_kernel, len(parts)),
        out_shape=jax.ShapeDtypeStruct((everyone, LANES), jnp.float32),
        grid_spec=pltpu.PrefetchScalarGridSpec(
            num_scalar_prefetch=1,
            grid=(2, observations // width),
            in_specs=[hx_spec] * len(parts) + [row_spec] * 3,
            out_specs=pl.BlockSpec((everyone, LANES), lambda g, i, me: (0, 0)),
            scratch_shapes=[pltpu.VMEM((everyone, width), jnp.float32)],
        ),
        compiler_params=pltpu.CompilerParams(dimension_semantics=("arbitrary", "arbitrary")),
        name="statistics",
    )(me, *parts, value, weight, live)


def transform_kernel(members, me_ref, stats_ref, transform_ref, mixer_ref, rest_ref):
    stats = stats_ref[...]
    everyone = stats.shape[0]
    gram = stats[:, :everyone]
    cross = stats[:, everyone : everyone + 1]
    misfit = stats[0:1, everyone + 1 : everyone + 2]
    total = stats[0:1, everyone + 2 : everyone + 3]
    dof = everyone - 1.0
    row = lax.broadcasted_iota(jnp.int32, (everyone, everyone), 0)
    col = lax.broadcasted_iota(jnp.int32, (everyone, everyone), 1)
    eye = (row == col).astype(jnp.float32)
    scl = dof / total
    gs = scl * gram
    bs = scl * cross
    qval = scl * misfit

    def whole_sum(x):
        return jnp.sum(jnp.sum(x, axis=1, keepdims=True), axis=0, keepdims=True)

    tval = whole_sum(gs * eye)
    rho = (1.0 + qval / dof) / (1.0 + tval / dof)
    amat = dof / rho * eye + gs
    scale = jnp.sqrt(whole_sum(amat * amat))

    def forward_step(_, carry):
        yn, zn = (split(x) for x in carry)
        tm = split(1.5 * eye - 0.5 * terms_dot(zn, yn))
        return terms_dot(yn, tm), terms_dot(tm, zn)

    _, zn = lax.fori_loop(0, ITERS, forward_step, (amat / scale, eye))
    parts = split(zn)
    pmat = terms_dot(parts, parts) / scale
    wide = jnp.broadcast_to(bs, (everyone, LANES))
    wbar = terms_dot(split(pmat), split(wide))[:, 0:1]
    transform = jnp.sqrt(dof) * zn / jnp.sqrt(scale) + wbar
    transform_ref[...] = transform
    held = pltpu.roll(transform, lax.rem(everyone - me_ref[0] * members, everyone), 0)
    mixer = held.T.astype(jnp.bfloat16)
    column_total = jnp.sum(mixer.astype(jnp.float32), axis=1, keepdims=True)
    extra = mixer_ref.shape[0] - everyone
    mixer_ref[...] = jnp.concatenate([mixer, jnp.ones((extra, everyone), jnp.bfloat16)], axis=0)
    rest_ref[...] = jnp.broadcast_to((1.0 - column_total) / everyone, rest_ref.shape)


def make_transform(stats, members, me):
    everyone = stats.shape[0]
    return pl.pallas_call(
        functools.partial(transform_kernel, members),
        out_shape=(
            jax.ShapeDtypeStruct((everyone, everyone), jnp.float32),
            jax.ShapeDtypeStruct((everyone + 16, everyone), jnp.bfloat16),
            jax.ShapeDtypeStruct((everyone, LANES), jnp.float32),
        ),
        in_specs=[pl.BlockSpec(memory_space=pltpu.SMEM), pl.BlockSpec(memory_space=pltpu.VMEM)],
        out_specs=(pl.BlockSpec(memory_space=pltpu.VMEM),) * 3,
        compiler_params=pltpu.CompilerParams(vmem_limit_bytes=VMEM),
        name="transform",
    )(me, stats)


def analysis_kernel(bounds, sources, aliased, base_ref, mixer_ref, rest_ref, own_ref, *refs):
    out_ref = refs[len(bounds) * sources + aliased]
    everyone, width = out_ref.shape
    members = own_ref.shape[0]
    step = pl.program_id(0)
    rest = rest_ref[:, 0:1]
    for i, (lo, hi) in enumerate(bounds):

        @pl.when((step >= lo) & (step < hi))
        def _(i=i, lo=lo):
            at = pl.ds(pl.multiple_of((step - lo) * width, width), width)
            cols = [own_ref[...]]
            cols += [ref[:, at] for ref in refs[i * sources : (i + 1) * sources]]
            if members % 16:
                cols = [x.astype(jnp.float32) for x in cols]
            cols = jnp.concatenate(cols, axis=0).astype(jnp.bfloat16)
            mixed = jnp.dot(mixer_ref[...], cols, preferred_element_type=jnp.float32)
            out = mixed[:everyone] + rest * mixed[everyone : everyone + 1]
            out_ref[...] = out.astype(out_ref.dtype)


def analyse(out, state, messages, mixer, rest, base, piece):
    members = state.shape[0]
    everyone = rest.shape[0]
    first, last = messages[0][0], messages[-1][1]
    width = 2 * piece // 8
    for lo, hi, _ in messages:
        width = math.gcd(width, hi - lo)
    skip = first // width
    whole = piece // width
    bounds = tuple((lo // width - skip, hi // width - skip) for lo, hi, _ in messages)
    received = [x for _, _, pieces in messages for x in pieces]
    aliased = int(out is not None)
    in_specs = [
        pl.BlockSpec(mixer.shape, lambda i, base: (0, 0)),
        pl.BlockSpec(rest.shape, lambda i, base: (0, 0)),
        pl.BlockSpec((members, width), lambda i, base: (0, base[0] * whole + skip + i)),
    ] + [pl.BlockSpec(memory_space=pltpu.VMEM)] * len(received)
    operands = [base, mixer, rest, state, *received]
    aliases = {}
    if aliased:
        in_specs.append(pl.BlockSpec(memory_space=pl.ANY))
        aliases = {len(operands): 0}
        operands.append(out)
    return pl.pallas_call(
        functools.partial(
            analysis_kernel, bounds, len(received) // len(messages), aliased
        ),
        out_shape=jax.ShapeDtypeStruct((everyone, piece), jnp.bfloat16),
        grid_spec=pltpu.PrefetchScalarGridSpec(
            num_scalar_prefetch=1,
            grid=((last - first) // width,),
            in_specs=in_specs,
            out_specs=pl.BlockSpec((everyone, width), lambda i, base: (0, skip + i)),
        ),
        input_output_aliases=aliases,
        compiler_params=pltpu.CompilerParams(
            dimension_semantics=("arbitrary",), vmem_limit_bytes=VMEM
        ),
        name="analysis",
    )(*operands)


def shards(state_a, state_b, obs_index, observation_count, obs_value, obs_weight):
    states = (state_a, state_b)
    members = state_a.shape[0]
    nmem = lax.axis_size("mem")
    ncol = lax.axis_size("col")
    piece = state_a.shape[1] // nmem
    nblk = obs_index.shape[1]
    slots = obs_index.shape[2]
    observations = nblk * slots
    unit = piece // 8
    me = lax.axis_index("mem")
    me_ref = me[None].astype(jnp.int32)
    shifts = range(1, nmem)

    def to_lower(array, shift):
        return lax.ppermute(array, "mem", [(i, (i - shift) % nmem) for i in range(nmem)])

    def to_upper(array, shift):
        return lax.ppermute(array, "mem", [(i, (i + shift) % nmem) for i in range(nmem)])

    def cut(message, source):
        group, lo, hi = message
        return [
            lax.dynamic_slice(
                source[group],
                (0, lax.rem(me + nmem - shift, nmem) * piece + lo * unit),
                (members, (hi - lo) * unit),
            )
            for shift in shifts
        ]

    others_index = [to_upper(obs_index, shift) for shift in shifts]
    index, *others_index = (
        x.reshape(2, observations // LANES, LANES) for x in (obs_index, *others_index)
    )

    own_hx = gather(state_a, state_b, index, me_ref, slots, piece)
    sent_hx = [
        gather(state_a, state_b, idx, lax.rem(me_ref + nmem - shift, nmem), slots, piece)
        for idx, shift in zip(others_index, shifts)
    ]
    got_hx = [to_lower(x, shift) for x, shift in zip(sent_hx, shifts)]

    live = (
        lax.broadcasted_iota(jnp.int32, (2, nblk, slots), 2) < observation_count[:, :, None]
    ).astype(jnp.float32)
    weight = (live * obs_weight).reshape(2, 1, observations)
    live = live.reshape(2, 1, observations)
    value = obs_value.reshape(2, 1, observations)
    stats = statistics([own_hx, *got_hx], value, weight, live, me_ref)

    received = []
    for i, message in enumerate(MESSAGES):
        if i < len(MESSAGES) - 1:
            pieces = cut(message, states)
        else:
            pieces = cut(message, lax.optimization_barrier((*states, stats)))
        received.append([to_lower(x, shift) for x, shift in zip(pieces, shifts)])

    def all_sum(x, axis, size):
        step = 1
        while step < size:
            x = x + lax.ppermute(x, axis, [(i, i ^ step) for i in range(size)])
            step *= 2
        return x

    stats = all_sum(all_sum(stats, "mem", nmem), "col", ncol)
    transform, mixer, rest = make_transform(stats, members, me_ref)

    outs = [None, None]
    for call in CALLS:
        group = MESSAGES[call[0]][0]
        messages = [
            (MESSAGES[m][1] * unit, MESSAGES[m][2] * unit, received[m]) for m in call
        ]
        outs[group] = analyse(
            outs[group], states[group], messages, mixer, rest, me_ref, piece
        )
    return (outs[0], outs[1], transform)


def solution(mesh):
    return jax.shard_map(
        shards,
        mesh=mesh,
        in_specs=(
            P("mem", "col"),
            P("mem", "col"),
            P(None, ("col", "mem"), None),
            P(None, ("col", "mem")),
            P(None, ("col", "mem"), None),
            P(None, ("col", "mem"), None),
        ),
        out_specs=(P(None, ("col", "mem")), P(None, ("col", "mem")), P()),
        check_vma=False,
    )
```

```python
import functools
import math

import jax
import jax.numpy as jnp
from jax import lax
from jax.experimental import pallas as pl
from jax.experimental.pallas import tpu as pltpu
from jax.sharding import PartitionSpec as P


ITERS = 24
VMEM = 16 * 1024 * 1024
LANES = 128

MESSAGES = (
    (0, 0, 3),
    (0, 3, 6),
    (0, 6, 8),
    (1, 0, 1),
    (1, 1, 4),
    (1, 4, 6),
    (1, 6, 8),
)
READ = (0, 1, 2)
SENT_GROUP = 1
CALLS = ((0, 1, 2), (3, 4), (5,), (6,))


def split(x):
    high = x.astype(jnp.bfloat16)
    rest = x - high.astype(jnp.float32)
    middle = rest.astype(jnp.bfloat16)
    return high, middle, (rest - middle.astype(jnp.float32)).astype(jnp.bfloat16)


def terms_dot(a, b):
    rows = a[0].shape[0]
    stacked = jnp.concatenate(a, axis=0)
    by_high = jnp.dot(stacked, b[0], preferred_element_type=jnp.float32)
    by_middle = jnp.dot(stacked[: 2 * rows], b[1], preferred_element_type=jnp.float32)
    by_low = jnp.dot(a[0], b[2], preferred_element_type=jnp.float32)
    second = by_high[rows : 2 * rows] + by_middle[:rows]
    third = by_high[2 * rows :] + by_middle[rows:] + by_low
    return by_high[:rows] + (second + third)


def take_rows(slots, ref, wanted_rows):
    per = LANES // slots
    rows = ref.shape[0]
    place = lax.broadcasted_iota(jnp.int32, (rows, LANES), 1) // slots
    for q, row in enumerate(wanted_rows):
        wanted = jnp.broadcast_to(row, (rows, LANES))
        acc = jnp.zeros((rows, LANES), jnp.float32)
        for j in range(per):
            start = (q * per + j) * LANES
            block = ref[:, start : start + LANES].astype(jnp.float32)
            taken = jnp.take_along_axis(block, wanted, axis=1, mode="promise_in_bounds")
            acc = jnp.where(place == j, taken, acc)
        yield q, acc


def gather_kernel(slots, groups, base_ref, index_ref, *refs):
    out_ref = refs[-1]
    lines = out_ref.shape[2] // LANES
    first = pl.program_id(0) * lines
    for i, group in enumerate(groups):
        rows = [index_ref[group, pl.ds(first + q, 1), :] for q in range(lines)]
        for q, taken in take_rows(slots, refs[i], rows):
            out_ref[i, :, q * LANES : (q + 1) * LANES] = taken.astype(out_ref.dtype)


def gather(states, groups, index, base, slots, piece):
    rows = states[0].shape[0]
    width = min(4096, piece)
    steps = piece // width
    observations = piece // LANES * slots
    state_spec = pl.BlockSpec((rows, width), lambda i, base: (0, base[0] * steps + i))
    return pl.pallas_call(
        functools.partial(gather_kernel, slots, groups),
        out_shape=jax.ShapeDtypeStruct((len(groups), rows, observations), jnp.bfloat16),
        grid_spec=pltpu.PrefetchScalarGridSpec(
            num_scalar_prefetch=1,
            grid=(steps,),
            in_specs=[pl.BlockSpec(index.shape, lambda i, base: (0, 0, 0))]
            + [state_spec] * len(groups),
            out_specs=pl.BlockSpec(
                (len(groups), rows, observations // steps), lambda i, base: (0, 0, i)
            ),
        ),
        compiler_params=pltpu.CompilerParams(dimension_semantics=("arbitrary",), vmem_limit_bytes=VMEM),
        name="gather",
    )(base, index, *[states[group] for group in groups])


def add_statistics(hx, value, wt, live, total_ref, so_far_ref):
    everyone = hx.shape[0]
    hmean = jnp.sum(hx, axis=0, keepdims=True) / everyone
    anomaly = hx - hmean
    innov = value - hmean
    scaled = anomaly * wt
    product = lax.dot_general(
        jnp.concatenate(split(scaled), axis=0),
        jnp.concatenate(split(anomaly), axis=0),
        (((1,), (1,)), ((), ())),
        preferred_element_type=jnp.float32,
    )

    def term(i, j):
        rows = product[i * everyone : (i + 1) * everyone]
        return rows[:, j * everyone : (j + 1) * everyone]

    gram = term(0, 0) + (term(0, 1) + term(1, 0) + (term(0, 2) + term(2, 0) + term(1, 1)))
    cross = jnp.sum(scaled * innov, axis=1, keepdims=True)
    misfit = jnp.sum(wt * innov * innov, axis=1, keepdims=True)
    count = jnp.sum(live, axis=1, keepdims=True)
    lane = lax.broadcasted_iota(jnp.int32, (everyone, LANES - everyone), 1)
    side = jnp.where(lane == 0, cross, jnp.where(lane == 1, misfit, jnp.where(lane == 2, count, 0.0)))
    new = jnp.concatenate([gram, side], axis=1)

    @pl.when(pl.program_id(0) == 0)
    def _():
        total_ref[...] = new if so_far_ref is None else so_far_ref[...] + new

    @pl.when(pl.program_id(0) > 0)
    def _():
        total_ref[...] += new


def statistics_kernel(parts, slots, group, first, lines, started, me_ref, *refs):
    part_refs = refs[:parts]
    refs = refs[parts:]
    value_ref, weight_ref, live_ref = refs[:3]
    refs = refs[3:]
    index_ref = None
    if lines:
        index_ref, *refs = refs
    so_far_ref = None
    if started:
        so_far_ref, *refs = refs
    total_ref, all_ref = refs
    members = part_refs[0].shape[-2]
    me = me_ref[0]

    def place(j):
        return pl.ds(pl.multiple_of(lax.rem(me + j, parts) * members, members), members)

    all_ref[place(0), :] = part_refs[0][0].astype(jnp.float32)
    for j in range(1, parts):
        if not lines:
            all_ref[place(j), :] = part_refs[j][0].astype(jnp.float32)
            continue
        at = first + pl.program_id(0) * lines
        rows = [index_ref[group, pl.ds(at + q, 1), :] for q in range(lines)]
        for q, taken in take_rows(slots, part_refs[j], rows):
            all_ref[place(j), q * LANES : (q + 1) * LANES] = taken
    add_statistics(
        all_ref[...], value_ref[0], weight_ref[0], live_ref[0], total_ref, so_far_ref
    )


def statistics(own, others, value, weight, live, me, group, lo, hi, so_far, index=None, slots=0):
    members = own.shape[1]
    parts = 1 + len(others)
    everyone = members * parts
    if index is None:
        width = math.gcd(hi - lo, 1024)
        lines = 0
        other_spec = pl.BlockSpec((1, members, width), lambda i, me: (0, 0, i))
    else:
        width = math.gcd(hi - lo, 512)
        lines = width // LANES
        other_spec = pl.BlockSpec(
            (members, width // slots * LANES), lambda i, me: (0, i)
        )
    skip = lo // width
    in_specs = [pl.BlockSpec((1, members, width), lambda i, me: (group, 0, skip + i))]
    in_specs += [other_spec] * len(others)
    in_specs += [pl.BlockSpec((1, 1, width), lambda i, me: (group, 0, skip + i))] * 3
    operands = [own, *others, value, weight, live]
    if index is not None:
        in_specs.append(pl.BlockSpec(index.shape, lambda i, me: (0, 0, 0)))
        operands.append(index)
    if so_far is not None:
        in_specs.append(pl.BlockSpec((everyone, LANES), lambda i, me: (0, 0)))
        operands.append(so_far)
    return pl.pallas_call(
        functools.partial(
            statistics_kernel, parts, slots, group, lo // LANES, lines, so_far is not None
        ),
        out_shape=jax.ShapeDtypeStruct((everyone, LANES), jnp.float32),
        grid_spec=pltpu.PrefetchScalarGridSpec(
            num_scalar_prefetch=1,
            grid=((hi - lo) // width,),
            in_specs=in_specs,
            out_specs=pl.BlockSpec((everyone, LANES), lambda i, me: (0, 0)),
            scratch_shapes=[pltpu.VMEM((everyone, width), jnp.float32)],
        ),
        compiler_params=pltpu.CompilerParams(dimension_semantics=("arbitrary",), vmem_limit_bytes=VMEM),
        name="statistics",
    )(me, *operands)


def transform_kernel(members, me_ref, stats_ref, transform_ref, mixer_ref, rest_ref):
    stats = stats_ref[...]
    everyone = stats.shape[0]
    gram = stats[:, :everyone]
    cross = stats[:, everyone : everyone + 1]
    misfit = stats[0:1, everyone + 1 : everyone + 2]
    total = stats[0:1, everyone + 2 : everyone + 3]
    dof = everyone - 1.0
    row = lax.broadcasted_iota(jnp.int32, (everyone, everyone), 0)
    col = lax.broadcasted_iota(jnp.int32, (everyone, everyone), 1)
    eye = (row == col).astype(jnp.float32)
    scl = dof / total
    gs = scl * gram
    bs = scl * cross
    qval = scl * misfit

    def whole_sum(x):
        return jnp.sum(jnp.sum(x, axis=1, keepdims=True), axis=0, keepdims=True)

    tval = whole_sum(gs * eye)
    rho = (1.0 + qval / dof) / (1.0 + tval / dof)
    amat = dof / rho * eye + gs
    scale = jnp.sqrt(whole_sum(amat * amat))

    def forward_step(_, carry):
        yn, zn = (split(x) for x in carry)
        tm = split(1.5 * eye - 0.5 * terms_dot(zn, yn))
        return terms_dot(yn, tm), terms_dot(tm, zn)

    _, zn = lax.fori_loop(0, ITERS, forward_step, (amat / scale, eye))
    parts = split(zn)
    pmat = terms_dot(parts, parts) / scale
    wide = jnp.broadcast_to(bs, (everyone, LANES))
    wbar = terms_dot(split(pmat), split(wide))[:, 0:1]
    transform = jnp.sqrt(dof) * zn / jnp.sqrt(scale) + wbar
    transform_ref[...] = transform
    held = pltpu.roll(transform, lax.rem(everyone - me_ref[0] * members, everyone), 0)
    mixer = held.T.astype(jnp.bfloat16)
    column_total = jnp.sum(mixer.astype(jnp.float32), axis=1, keepdims=True)
    extra = mixer_ref.shape[0] - everyone
    mixer_ref[...] = jnp.concatenate([mixer, jnp.ones((extra, everyone), jnp.bfloat16)], axis=0)
    rest_ref[...] = jnp.broadcast_to((1.0 - column_total) / everyone, rest_ref.shape)


def make_transform(stats, members, me):
    everyone = stats.shape[0]
    return pl.pallas_call(
        functools.partial(transform_kernel, members),
        out_shape=(
            jax.ShapeDtypeStruct((everyone, everyone), jnp.float32),
            jax.ShapeDtypeStruct((everyone + 16, everyone), jnp.bfloat16),
            jax.ShapeDtypeStruct((everyone, LANES), jnp.float32),
        ),
        in_specs=[pl.BlockSpec(memory_space=pltpu.SMEM), pl.BlockSpec(memory_space=pltpu.VMEM)],
        out_specs=(pl.BlockSpec(memory_space=pltpu.VMEM),) * 3,
        compiler_params=pltpu.CompilerParams(vmem_limit_bytes=VMEM),
        name="transform",
    )(me, stats)


def analysis_kernel(bounds, sources, aliased, base_ref, mixer_ref, rest_ref, own_ref, *refs):
    out_ref = refs[len(bounds) * sources + aliased]
    everyone, width = out_ref.shape
    members = own_ref.shape[0]
    step = pl.program_id(0)
    rest = rest_ref[:, 0:1]
    for i, (lo, hi) in enumerate(bounds):

        @pl.when((step >= lo) & (step < hi))
        def _(i=i, lo=lo):
            at = pl.ds(pl.multiple_of((step - lo) * width, width), width)
            cols = [own_ref[...]]
            cols += [ref[:, at] for ref in refs[i * sources : (i + 1) * sources]]
            if members % 16:
                cols = [x.astype(jnp.float32) for x in cols]
            cols = jnp.concatenate(cols, axis=0).astype(jnp.bfloat16)
            mixed = jnp.dot(mixer_ref[...], cols, preferred_element_type=jnp.float32)
            out = mixed[:everyone] + rest * mixed[everyone : everyone + 1]
            out_ref[...] = out.astype(out_ref.dtype)


def analyse(out, state, messages, mixer, rest, base, piece):
    members = state.shape[0]
    everyone = rest.shape[0]
    first, last = messages[0][0], messages[-1][1]
    width = 2 * piece // 8
    for lo, hi, _ in messages:
        width = math.gcd(width, hi - lo)
    skip = first // width
    whole = piece // width
    bounds = tuple((lo // width - skip, hi // width - skip) for lo, hi, _ in messages)
    received = [x for _, _, pieces in messages for x in pieces]
    aliased = int(out is not None)
    in_specs = [
        pl.BlockSpec(mixer.shape, lambda i, base: (0, 0)),
        pl.BlockSpec(rest.shape, lambda i, base: (0, 0)),
        pl.BlockSpec((members, width), lambda i, base: (0, base[0] * whole + skip + i)),
    ] + [pl.BlockSpec(memory_space=pltpu.VMEM)] * len(received)
    operands = [base, mixer, rest, state, *received]
    aliases = {}
    if aliased:
        in_specs.append(pl.BlockSpec(memory_space=pl.ANY))
        aliases = {len(operands): 0}
        operands.append(out)
    return pl.pallas_call(
        functools.partial(
            analysis_kernel, bounds, len(received) // len(messages), aliased
        ),
        out_shape=jax.ShapeDtypeStruct((everyone, piece), jnp.bfloat16),
        grid_spec=pltpu.PrefetchScalarGridSpec(
            num_scalar_prefetch=1,
            grid=((last - first) // width,),
            in_specs=in_specs,
            out_specs=pl.BlockSpec((everyone, width), lambda i, base: (0, skip + i)),
        ),
        input_output_aliases=aliases,
        compiler_params=pltpu.CompilerParams(
            dimension_semantics=("arbitrary",), vmem_limit_bytes=VMEM
        ),
        name="analysis",
    )(*operands)


def shards(state_a, state_b, obs_index, observation_count, obs_value, obs_weight):
    states = (state_a, state_b)
    members = state_a.shape[0]
    nmem = lax.axis_size("mem")
    ncol = lax.axis_size("col")
    piece = state_a.shape[1] // nmem
    nblk = obs_index.shape[1]
    slots = obs_index.shape[2]
    observations = nblk * slots
    unit = piece // 8
    me = lax.axis_index("mem")
    me_ref = me[None].astype(jnp.int32)
    shifts = range(1, nmem)

    def to_lower(array, shift):
        return lax.ppermute(array, "mem", [(i, (i - shift) % nmem) for i in range(nmem)])

    def to_upper(array, shift):
        return lax.ppermute(array, "mem", [(i, (i + shift) % nmem) for i in range(nmem)])

    def cut(message, source):
        group, lo, hi = message
        return [
            lax.dynamic_slice(
                source[group],
                (0, lax.rem(me + nmem - shift, nmem) * piece + lo * unit),
                (members, (hi - lo) * unit),
            )
            for shift in shifts
        ]

    others_index = [to_upper(obs_index, shift) for shift in shifts]
    index, *others_index = (
        x.reshape(2, observations // LANES, LANES) for x in (obs_index, *others_index)
    )

    own_hx = gather(states, (0, 1), index, me_ref, slots, piece)
    sent_hx = [
        gather(
            states, (SENT_GROUP,), idx, lax.rem(me_ref + nmem - shift, nmem), slots, piece
        )
        for idx, shift in zip(others_index, shifts)
    ]
    got_hx = [to_lower(x, shift) for x, shift in zip(sent_hx, shifts)]

    live = (
        lax.broadcasted_iota(jnp.int32, (2, nblk, slots), 2) < observation_count[:, :, None]
    ).astype(jnp.float32)
    weight = (live * obs_weight).reshape(2, 1, observations)
    live = live.reshape(2, 1, observations)
    value = obs_value.reshape(2, 1, observations)

    received = {}

    def send(i, pieces):
        received[i] = [to_lower(x, shift) for x, shift in zip(pieces, shifts)]

    for i, message in enumerate(MESSAGES[:-1]):
        pieces = cut(message, states)
        send(i, pieces)

    def read(i, so_far):
        group, lo, hi = MESSAGES[i]
        lo, hi = (x * observations // 8 for x in (lo, hi))
        return statistics(
            own_hx, received[i], value, weight, live, me_ref, group, lo, hi, so_far, index, slots
        )

    stats = read(READ[0], None)
    stats = statistics(
        own_hx, got_hx, value, weight, live, me_ref, SENT_GROUP, 0, observations, stats
    )
    for i in READ[1:]:
        stats = read(i, stats)

    pieces = cut(MESSAGES[-1], lax.optimization_barrier((*states, stats)))
    send(len(MESSAGES) - 1, pieces)

    def all_sum(x, axis, size):
        step = 1
        while step < size:
            x = x + lax.ppermute(x, axis, [(i, i ^ step) for i in range(size)])
            step *= 2
        return x

    stats = all_sum(all_sum(stats, "mem", nmem), "col", ncol)
    transform, mixer, rest = make_transform(stats, members, me_ref)

    outs = [None, None]
    for call in CALLS:
        group = MESSAGES[call[0]][0]
        messages = [
            (MESSAGES[m][1] * unit, MESSAGES[m][2] * unit, received[m]) for m in call
        ]
        outs[group] = analyse(
            outs[group], states[group], messages, mixer, rest, me_ref, piece
        )
    return (outs[0], outs[1], transform)


def solution(mesh):
    return jax.shard_map(
        shards,
        mesh=mesh,
        in_specs=(
            P("mem", "col"),
            P("mem", "col"),
            P(None, ("col", "mem"), None),
            P(None, ("col", "mem")),
            P(None, ("col", "mem"), None),
            P(None, ("col", "mem"), None),
        ),
        out_specs=(P(None, ("col", "mem")), P(None, ("col", "mem")), P()),
        check_vma=False,
    )
```

```python
import functools
import math

import jax
import jax.numpy as jnp
from jax import lax
from jax.experimental import pallas as pl
from jax.experimental.pallas import tpu as pltpu
from jax.sharding import PartitionSpec as P


ITERS = 24
VMEM = 16 * 1024 * 1024
MOST_VMEM = 50 * 1024 * 1024
LANES = 128

MESSAGES = (
    (0, 0, 2),
    (0, 2, 4),
    (0, 4, 6),
    (0, 6, 8),
    (1, 0, 1),
    (1, 1, 2),
    (1, 2, 5),
    (1, 5, 7),
    (1, 7, 8),
)
READ = (0, 1, 2, 3, 4)
SENT = (1, 1)
CALLS = ((0, 1, 2, 3), (4, 5, 6), (7,), (8,))


def split(x):
    high = x.astype(jnp.bfloat16)
    rest = x - high.astype(jnp.float32)
    middle = rest.astype(jnp.bfloat16)
    return high, middle, (rest - middle.astype(jnp.float32)).astype(jnp.bfloat16)


def terms_dot(a, b):
    rows = a[0].shape[0]
    stacked = jnp.concatenate(a, axis=0)
    by_high = jnp.dot(stacked, b[0], preferred_element_type=jnp.float32)
    by_middle = jnp.dot(stacked[: 2 * rows], b[1], preferred_element_type=jnp.float32)
    by_low = jnp.dot(a[0], b[2], preferred_element_type=jnp.float32)
    second = by_high[rows : 2 * rows] + by_middle[:rows]
    third = by_high[2 * rows :] + by_middle[rows:] + by_low
    return by_high[:rows] + (second + third)


def cut_kernel(base_ref, state_ref, out_ref):
    out_ref[...] = state_ref[...]


def cut_first(state, base, lo, hi, piece):
    members, length = state.shape[0], hi - lo
    whole = piece // length
    return pl.pallas_call(
        cut_kernel,
        out_shape=jax.ShapeDtypeStruct((members, length), state.dtype),
        grid_spec=pltpu.PrefetchScalarGridSpec(
            num_scalar_prefetch=1,
            grid=(1,),
            in_specs=[
                pl.BlockSpec((members, length), lambda i, base: (0, base[0] * whole + lo // length))
            ],
            out_specs=pl.BlockSpec(memory_space=pltpu.VMEM),
        ),
        compiler_params=pltpu.CompilerParams(vmem_limit_bytes=MOST_VMEM),
        name="cut",
    )(base, state)


def take_rows(slots, ref, wanted_rows):
    per = LANES // slots
    rows = ref.shape[0]
    place = lax.broadcasted_iota(jnp.int32, (rows, LANES), 1) // slots
    for q, row in enumerate(wanted_rows):
        wanted = jnp.broadcast_to(row, (rows, LANES))
        acc = jnp.zeros((rows, LANES), jnp.float32)
        for j in range(per):
            start = (q * per + j) * LANES
            block = ref[:, start : start + LANES].astype(jnp.float32)
            taken = jnp.take_along_axis(block, wanted, axis=1, mode="promise_in_bounds")
            acc = jnp.where(place == j, taken, acc)
        yield q, acc


def gather_kernel(slots, groups, skip, base_ref, index_ref, *refs):
    out_ref = refs[-1]
    lines = out_ref.shape[2] // LANES
    first = (skip + pl.program_id(0)) * lines
    for i, group in enumerate(groups):
        rows = [index_ref[group, pl.ds(first + q, 1), :] for q in range(lines)]
        for q, taken in take_rows(slots, refs[i], rows):
            out_ref[i, :, q * LANES : (q + 1) * LANES] = taken.astype(out_ref.dtype)


def gather(states, groups, index, base, slots, piece, eighth=0):
    rows = states[0].shape[0]
    width = piece // 8
    steps = 8 - eighth
    observations = width // LANES * slots * steps
    state_spec = pl.BlockSpec((rows, width), lambda i, base: (0, base[0] * 8 + eighth + i))
    return pl.pallas_call(
        functools.partial(gather_kernel, slots, groups, eighth),
        out_shape=jax.ShapeDtypeStruct((len(groups), rows, observations), jnp.bfloat16),
        grid_spec=pltpu.PrefetchScalarGridSpec(
            num_scalar_prefetch=1,
            grid=(steps,),
            in_specs=[pl.BlockSpec(index.shape, lambda i, base: (0, 0, 0))]
            + [state_spec] * len(groups),
            out_specs=pl.BlockSpec(
                (len(groups), rows, observations // steps), lambda i, base: (0, 0, i)
            ),
        ),
        compiler_params=pltpu.CompilerParams(dimension_semantics=("arbitrary",), vmem_limit_bytes=VMEM),
        name="gather",
    )(base, index, *[states[group] for group in groups])


def add_statistics(hx, value, wt, live, total_ref, so_far_ref):
    everyone = hx.shape[0]
    hmean = jnp.sum(hx, axis=0, keepdims=True) / everyone
    anomaly = hx - hmean
    innov = value - hmean
    scaled = anomaly * wt
    product = lax.dot_general(
        jnp.concatenate(split(scaled), axis=0),
        jnp.concatenate(split(anomaly), axis=0),
        (((1,), (1,)), ((), ())),
        preferred_element_type=jnp.float32,
    )

    def term(i, j):
        rows = product[i * everyone : (i + 1) * everyone]
        return rows[:, j * everyone : (j + 1) * everyone]

    gram = term(0, 0) + (term(0, 1) + term(1, 0) + (term(0, 2) + term(2, 0) + term(1, 1)))
    cross = jnp.sum(scaled * innov, axis=1, keepdims=True)
    misfit = jnp.sum(wt * innov * innov, axis=1, keepdims=True)
    count = jnp.sum(live, axis=1, keepdims=True)
    lane = lax.broadcasted_iota(jnp.int32, (everyone, LANES - everyone), 1)
    side = jnp.where(lane == 0, cross, jnp.where(lane == 1, misfit, jnp.where(lane == 2, count, 0.0)))
    new = jnp.concatenate([gram, side], axis=1)

    @pl.when(pl.program_id(0) == 0)
    def _():
        total_ref[...] = new if so_far_ref is None else so_far_ref[...] + new

    @pl.when(pl.program_id(0) > 0)
    def _():
        total_ref[...] += new


def statistics_kernel(parts, slots, group, first, lines, started, me_ref, *refs):
    part_refs = refs[:parts]
    refs = refs[parts:]
    value_ref, weight_ref, live_ref = refs[:3]
    refs = refs[3:]
    index_ref = None
    if lines:
        index_ref, *refs = refs
    so_far_ref = None
    if started:
        so_far_ref, *refs = refs
    total_ref, all_ref = refs
    members = part_refs[0].shape[-2]
    me = me_ref[0]

    def place(j):
        return pl.ds(pl.multiple_of(lax.rem(me + j, parts) * members, members), members)

    all_ref[place(0), :] = part_refs[0][0].astype(jnp.float32)
    for j in range(1, parts):
        if not lines:
            all_ref[place(j), :] = part_refs[j][0].astype(jnp.float32)
            continue
        at = first + pl.program_id(0) * lines
        rows = [index_ref[group, pl.ds(at + q, 1), :] for q in range(lines)]
        for q, taken in take_rows(slots, part_refs[j], rows):
            all_ref[place(j), q * LANES : (q + 1) * LANES] = taken
    add_statistics(
        all_ref[...], value_ref[0], weight_ref[0], live_ref[0], total_ref, so_far_ref
    )


def statistics(own, others, value, weight, live, me, group, lo, hi, so_far, index=None, slots=0):
    members = own.shape[1]
    parts = 1 + len(others)
    everyone = members * parts
    if index is None:
        width = math.gcd(math.gcd(lo, hi), 1024)
        lines = 0
        other_spec = pl.BlockSpec((1, members, width), lambda i, me: (0, 0, i))
    else:
        width = math.gcd(math.gcd(lo, hi), 512)
        lines = width // LANES
        other_spec = pl.BlockSpec(
            (members, width // slots * LANES), lambda i, me: (0, i)
        )
    skip = lo // width
    in_specs = [pl.BlockSpec((1, members, width), lambda i, me: (group, 0, skip + i))]
    in_specs += [other_spec] * len(others)
    in_specs += [pl.BlockSpec((1, 1, width), lambda i, me: (group, 0, skip + i))] * 3
    operands = [own, *others, value, weight, live]
    if index is not None:
        in_specs.append(pl.BlockSpec(index.shape, lambda i, me: (0, 0, 0)))
        operands.append(index)
    if so_far is not None:
        in_specs.append(pl.BlockSpec((everyone, LANES), lambda i, me: (0, 0)))
        operands.append(so_far)
    return pl.pallas_call(
        functools.partial(
            statistics_kernel, parts, slots, group, lo // LANES, lines, so_far is not None
        ),
        out_shape=jax.ShapeDtypeStruct((everyone, LANES), jnp.float32),
        grid_spec=pltpu.PrefetchScalarGridSpec(
            num_scalar_prefetch=1,
            grid=((hi - lo) // width,),
            in_specs=in_specs,
            out_specs=pl.BlockSpec((everyone, LANES), lambda i, me: (0, 0)),
            scratch_shapes=[pltpu.VMEM((everyone, width), jnp.float32)],
        ),
        compiler_params=pltpu.CompilerParams(dimension_semantics=("arbitrary",), vmem_limit_bytes=VMEM),
        name="statistics",
    )(me, *operands)


def transform_kernel(members, me_ref, stats_ref, transform_ref, mixer_ref, rest_ref):
    stats = stats_ref[...]
    everyone = stats.shape[0]
    gram = stats[:, :everyone]
    cross = stats[:, everyone : everyone + 1]
    misfit = stats[0:1, everyone + 1 : everyone + 2]
    total = stats[0:1, everyone + 2 : everyone + 3]
    dof = everyone - 1.0
    row = lax.broadcasted_iota(jnp.int32, (everyone, everyone), 0)
    col = lax.broadcasted_iota(jnp.int32, (everyone, everyone), 1)
    eye = (row == col).astype(jnp.float32)
    scl = dof / total
    gs = scl * gram
    bs = scl * cross
    qval = scl * misfit

    def whole_sum(x):
        return jnp.sum(jnp.sum(x, axis=1, keepdims=True), axis=0, keepdims=True)

    tval = whole_sum(gs * eye)
    rho = (1.0 + qval / dof) / (1.0 + tval / dof)
    amat = dof / rho * eye + gs
    scale = jnp.sqrt(whole_sum(amat * amat))

    def forward_step(_, carry):
        yn, zn = (split(x) for x in carry)
        tm = split(1.5 * eye - 0.5 * terms_dot(zn, yn))
        return terms_dot(yn, tm), terms_dot(tm, zn)

    _, zn = lax.fori_loop(0, ITERS, forward_step, (amat / scale, eye))
    parts = split(zn)
    pmat = terms_dot(parts, parts) / scale
    wide = jnp.broadcast_to(bs, (everyone, LANES))
    wbar = terms_dot(split(pmat), split(wide))[:, 0:1]
    transform = jnp.sqrt(dof) * zn / jnp.sqrt(scale) + wbar
    transform_ref[...] = transform
    held = pltpu.roll(transform, lax.rem(everyone - me_ref[0] * members, everyone), 0)
    mixer = held.T.astype(jnp.bfloat16)
    column_total = jnp.sum(mixer.astype(jnp.float32), axis=1, keepdims=True)
    extra = mixer_ref.shape[0] - everyone
    mixer_ref[...] = jnp.concatenate([mixer, jnp.ones((extra, everyone), jnp.bfloat16)], axis=0)
    rest_ref[...] = jnp.broadcast_to((1.0 - column_total) / everyone, rest_ref.shape)


def make_transform(stats, members, me):
    everyone = stats.shape[0]
    return pl.pallas_call(
        functools.partial(transform_kernel, members),
        out_shape=(
            jax.ShapeDtypeStruct((everyone, everyone), jnp.float32),
            jax.ShapeDtypeStruct((everyone + 16, everyone), jnp.bfloat16),
            jax.ShapeDtypeStruct((everyone, LANES), jnp.float32),
        ),
        in_specs=[pl.BlockSpec(memory_space=pltpu.SMEM), pl.BlockSpec(memory_space=pltpu.VMEM)],
        out_specs=(pl.BlockSpec(memory_space=pltpu.VMEM),) * 3,
        compiler_params=pltpu.CompilerParams(vmem_limit_bytes=VMEM),
        name="transform",
    )(me, stats)


def analysis_kernel(bounds, sources, aliased, base_ref, mixer_ref, rest_ref, own_ref, *refs):
    out_ref = refs[len(bounds) * sources + aliased]
    everyone, width = out_ref.shape
    members = own_ref.shape[0]
    step = pl.program_id(0)
    rest = rest_ref[:, 0:1]
    for i, (lo, hi) in enumerate(bounds):

        @pl.when((step >= lo) & (step < hi))
        def _(i=i, lo=lo):
            at = pl.ds(pl.multiple_of((step - lo) * width, width), width)
            cols = [own_ref[...]]
            cols += [ref[:, at] for ref in refs[i * sources : (i + 1) * sources]]
            if members % 16:
                cols = [x.astype(jnp.float32) for x in cols]
            cols = jnp.concatenate(cols, axis=0).astype(jnp.bfloat16)
            mixed = jnp.dot(mixer_ref[...], cols, preferred_element_type=jnp.float32)
            out = mixed[:everyone] + rest * mixed[everyone : everyone + 1]
            out_ref[...] = out.astype(out_ref.dtype)


def analyse(out, state, messages, mixer, rest, base, piece):
    members = state.shape[0]
    everyone = rest.shape[0]
    first, last = messages[0][0], messages[-1][1]
    width = 2 * piece // 8
    for lo, hi, _ in messages:
        width = math.gcd(width, lo, hi)
    skip = first // width
    whole = piece // width
    bounds = tuple((lo // width - skip, hi // width - skip) for lo, hi, _ in messages)
    received = [x for _, _, pieces in messages for x in pieces]
    aliased = int(out is not None)
    in_specs = [
        pl.BlockSpec(mixer.shape, lambda i, base: (0, 0)),
        pl.BlockSpec(rest.shape, lambda i, base: (0, 0)),
        pl.BlockSpec((members, width), lambda i, base: (0, base[0] * whole + skip + i)),
    ] + [pl.BlockSpec(memory_space=pltpu.VMEM)] * len(received)
    operands = [base, mixer, rest, state, *received]
    aliases = {}
    if aliased:
        in_specs.append(pl.BlockSpec(memory_space=pl.ANY))
        aliases = {len(operands): 0}
        operands.append(out)
    return pl.pallas_call(
        functools.partial(
            analysis_kernel, bounds, len(received) // len(messages), aliased
        ),
        out_shape=jax.ShapeDtypeStruct((everyone, piece), jnp.bfloat16),
        grid_spec=pltpu.PrefetchScalarGridSpec(
            num_scalar_prefetch=1,
            grid=((last - first) // width,),
            in_specs=in_specs,
            out_specs=pl.BlockSpec((everyone, width), lambda i, base: (0, skip + i)),
        ),
        input_output_aliases=aliases,
        compiler_params=pltpu.CompilerParams(
            dimension_semantics=("arbitrary",), vmem_limit_bytes=VMEM
        ),
        name="analysis",
    )(*operands)


def shards(state_a, state_b, obs_index, observation_count, obs_value, obs_weight):
    states = (state_a, state_b)
    members = state_a.shape[0]
    nmem = lax.axis_size("mem")
    ncol = lax.axis_size("col")
    piece = state_a.shape[1] // nmem
    nblk = obs_index.shape[1]
    slots = obs_index.shape[2]
    observations = nblk * slots
    unit = piece // 8
    me = lax.axis_index("mem")
    me_ref = me[None].astype(jnp.int32)
    shifts = range(1, nmem)

    def to_lower(array, shift):
        return lax.ppermute(array, "mem", [(i, (i - shift) % nmem) for i in range(nmem)])

    def to_upper(array, shift):
        return lax.ppermute(array, "mem", [(i, (i + shift) % nmem) for i in range(nmem)])

    def cut(message, source):
        group, lo, hi = message
        return [
            lax.dynamic_slice(
                source[group],
                (0, lax.rem(me + nmem - shift, nmem) * piece + lo * unit),
                (members, (hi - lo) * unit),
            )
            for shift in shifts
        ]

    others_index = [to_upper(obs_index, shift) for shift in shifts]
    index, *others_index = (
        x.reshape(2, observations // LANES, LANES) for x in (obs_index, *others_index)
    )

    group, lo, hi = MESSAGES[0]
    first_pieces = [
        cut_first(states[group], lax.rem(me_ref + nmem - shift, nmem), lo * unit, hi * unit, piece)
        for shift in shifts
    ]
    own_hx = gather(states, (0, 1), index, me_ref, slots, piece)
    sent_hx = [
        gather(states, SENT[:1], idx, lax.rem(me_ref + nmem - shift, nmem), slots, piece, SENT[1])
        for idx, shift in zip(others_index, shifts)
    ]
    got_hx = [to_lower(x, shift) for x, shift in zip(sent_hx, shifts)]

    live = (
        lax.broadcasted_iota(jnp.int32, (2, nblk, slots), 2) < observation_count[:, :, None]
    ).astype(jnp.float32)
    weight = (live * obs_weight).reshape(2, 1, observations)
    live = live.reshape(2, 1, observations)
    value = obs_value.reshape(2, 1, observations)

    received = {}

    def send(i, pieces):
        received[i] = [to_lower(x, shift) for x, shift in zip(pieces, shifts)]

    send(0, first_pieces)
    sources = lax.optimization_barrier((*states, sent_hx))
    for i, message in enumerate(MESSAGES[1:-1], 1):
        pieces = cut(message, sources)
        send(i, pieces)

    def read(i, so_far):
        group, lo, hi = MESSAGES[i]
        lo, hi = (x * observations // 8 for x in (lo, hi))
        return statistics(
            own_hx, received[i], value, weight, live, me_ref, group, lo, hi, so_far, index, slots
        )

    stats = read(READ[0], None)
    stats = statistics(
        own_hx,
        got_hx,
        value,
        weight,
        live,
        me_ref,
        SENT[0],
        SENT[1] * observations // 8,
        observations,
        stats,
    )
    for i in READ[1:]:
        stats = read(i, stats)

    pieces = cut(MESSAGES[-1], lax.optimization_barrier((*states, stats)))
    send(len(MESSAGES) - 1, pieces)

    def all_sum(x, axis, size):
        step = 1
        while step < size:
            x = x + lax.ppermute(x, axis, [(i, i ^ step) for i in range(size)])
            step *= 2
        return x

    stats = all_sum(all_sum(stats, "mem", nmem), "col", ncol)
    transform, mixer, rest = make_transform(stats, members, me_ref)

    outs = [None, None]
    for call in CALLS:
        group = MESSAGES[call[0]][0]
        messages = [
            (MESSAGES[m][1] * unit, MESSAGES[m][2] * unit, received[m]) for m in call
        ]
        outs[group] = analyse(
            outs[group], states[group], messages, mixer, rest, me_ref, piece
        )
    return (outs[0], outs[1], transform)


def solution(mesh):
    return jax.shard_map(
        shards,
        mesh=mesh,
        in_specs=(
            P("mem", "col"),
            P("mem", "col"),
            P(None, ("col", "mem"), None),
            P(None, ("col", "mem")),
            P(None, ("col", "mem"), None),
            P(None, ("col", "mem"), None),
        ),
        out_specs=(P(None, ("col", "mem")), P(None, ("col", "mem")), P()),
        check_vma=False,
    )
```

```python
import functools
import math

import jax
import jax.numpy as jnp
from jax import lax
from jax.experimental import pallas as pl
from jax.experimental.pallas import tpu as pltpu
from jax.sharding import PartitionSpec as P


ITERS = 24
VMEM = 16 * 1024 * 1024
MOST_VMEM = 50 * 1024 * 1024
LANES = 128

MESSAGES = (
    (0, 0, 8),
    (0, 8, 16),
    (0, 16, 24),
    (0, 24, 32),
    (1, 0, 4),
    (1, 4, 6),
    (1, 6, 20),
    (1, 20, 28),
    (1, 28, 32),
)
READ = (0, 1, 2, 3, 4)
SENT = (1, 1)
CALLS = ((0, 1, 2, 3), (4, 5, 6), (7,), (8,))


def split(x):
    high = x.astype(jnp.bfloat16)
    rest = x - high.astype(jnp.float32)
    middle = rest.astype(jnp.bfloat16)
    return high, middle, (rest - middle.astype(jnp.float32)).astype(jnp.bfloat16)


def terms_dot(a, b):
    rows = a[0].shape[0]
    stacked = jnp.concatenate(a, axis=0)
    by_high = jnp.dot(stacked, b[0], preferred_element_type=jnp.float32)
    by_middle = jnp.dot(stacked[: 2 * rows], b[1], preferred_element_type=jnp.float32)
    by_low = jnp.dot(a[0], b[2], preferred_element_type=jnp.float32)
    second = by_high[rows : 2 * rows] + by_middle[:rows]
    third = by_high[2 * rows :] + by_middle[rows:] + by_low
    return by_high[:rows] + (second + third)


def cut_kernel(base_ref, state_ref, out_ref):
    out_ref[...] = state_ref[...]


def cut_first(state, base, lo, hi, piece):
    members, length = state.shape[0], hi - lo
    whole = piece // length
    return pl.pallas_call(
        cut_kernel,
        out_shape=jax.ShapeDtypeStruct((members, length), state.dtype),
        grid_spec=pltpu.PrefetchScalarGridSpec(
            num_scalar_prefetch=1,
            grid=(1,),
            in_specs=[
                pl.BlockSpec((members, length), lambda i, base: (0, base[0] * whole + lo // length))
            ],
            out_specs=pl.BlockSpec(memory_space=pltpu.VMEM),
        ),
        compiler_params=pltpu.CompilerParams(vmem_limit_bytes=MOST_VMEM),
        name="cut",
    )(base, state)


def take_rows(slots, ref, wanted_rows):
    per = LANES // slots
    rows = ref.shape[0]
    place = lax.broadcasted_iota(jnp.int32, (rows, LANES), 1) // slots
    for q, row in enumerate(wanted_rows):
        wanted = jnp.broadcast_to(row, (rows, LANES))
        acc = jnp.zeros((rows, LANES), jnp.float32)
        for j in range(per):
            start = (q * per + j) * LANES
            block = ref[:, start : start + LANES].astype(jnp.float32)
            taken = jnp.take_along_axis(block, wanted, axis=1, mode="promise_in_bounds")
            acc = jnp.where(place == j, taken, acc)
        yield q, acc


def gather_kernel(slots, groups, skip, base_ref, index_ref, *refs):
    out_ref = refs[-1]
    lines = out_ref.shape[2] // LANES
    first = (skip + pl.program_id(0)) * lines
    for i, group in enumerate(groups):
        rows = [index_ref[group, pl.ds(first + q, 1), :] for q in range(lines)]
        for q, taken in take_rows(slots, refs[i], rows):
            out_ref[i, :, q * LANES : (q + 1) * LANES] = taken.astype(out_ref.dtype)


def gather(states, groups, index, base, slots, piece, eighth=0):
    rows = states[0].shape[0]
    width = piece // 8
    steps = 8 - eighth
    observations = width // LANES * slots * steps
    state_spec = pl.BlockSpec((rows, width), lambda i, base: (0, base[0] * 8 + eighth + i))
    return pl.pallas_call(
        functools.partial(gather_kernel, slots, groups, eighth),
        out_shape=jax.ShapeDtypeStruct((len(groups), rows, observations), jnp.bfloat16),
        grid_spec=pltpu.PrefetchScalarGridSpec(
            num_scalar_prefetch=1,
            grid=(steps,),
            in_specs=[pl.BlockSpec(index.shape, lambda i, base: (0, 0, 0))]
            + [state_spec] * len(groups),
            out_specs=pl.BlockSpec(
                (len(groups), rows, observations // steps), lambda i, base: (0, 0, i)
            ),
        ),
        compiler_params=pltpu.CompilerParams(dimension_semantics=("arbitrary",), vmem_limit_bytes=VMEM),
        name="gather",
    )(base, index, *[states[group] for group in groups])


def add_statistics(hx, value, wt, live, total_ref, so_far_ref):
    everyone = hx.shape[0]
    hmean = jnp.sum(hx, axis=0, keepdims=True) / everyone
    anomaly = hx - hmean
    innov = value - hmean
    scaled = anomaly * wt
    product = lax.dot_general(
        jnp.concatenate(split(scaled), axis=0),
        jnp.concatenate(split(anomaly), axis=0),
        (((1,), (1,)), ((), ())),
        preferred_element_type=jnp.float32,
    )

    def term(i, j):
        rows = product[i * everyone : (i + 1) * everyone]
        return rows[:, j * everyone : (j + 1) * everyone]

    gram = term(0, 0) + (term(0, 1) + term(1, 0) + (term(0, 2) + term(2, 0) + term(1, 1)))
    cross = jnp.sum(scaled * innov, axis=1, keepdims=True)
    misfit = jnp.sum(wt * innov * innov, axis=1, keepdims=True)
    count = jnp.sum(live, axis=1, keepdims=True)
    lane = lax.broadcasted_iota(jnp.int32, (everyone, LANES - everyone), 1)
    side = jnp.where(lane == 0, cross, jnp.where(lane == 1, misfit, jnp.where(lane == 2, count, 0.0)))
    new = jnp.concatenate([gram, side], axis=1)

    @pl.when(pl.program_id(0) == 0)
    def _():
        total_ref[...] = new if so_far_ref is None else so_far_ref[...] + new

    @pl.when(pl.program_id(0) > 0)
    def _():
        total_ref[...] += new


def statistics_kernel(parts, slots, group, first, lines, started, me_ref, *refs):
    part_refs = refs[:parts]
    refs = refs[parts:]
    value_ref, weight_ref, live_ref = refs[:3]
    refs = refs[3:]
    index_ref = None
    if lines:
        index_ref, *refs = refs
    so_far_ref = None
    if started:
        so_far_ref, *refs = refs
    total_ref, all_ref = refs
    members = part_refs[0].shape[-2]
    me = me_ref[0]

    def place(j):
        return pl.ds(pl.multiple_of(lax.rem(me + j, parts) * members, members), members)

    all_ref[place(0), :] = part_refs[0][0].astype(jnp.float32)
    for j in range(1, parts):
        if not lines:
            all_ref[place(j), :] = part_refs[j][0].astype(jnp.float32)
            continue
        at = first + pl.program_id(0) * lines
        rows = [index_ref[group, pl.ds(at + q, 1), :] for q in range(lines)]
        for q, taken in take_rows(slots, part_refs[j], rows):
            all_ref[place(j), q * LANES : (q + 1) * LANES] = taken
    add_statistics(
        all_ref[...], value_ref[0], weight_ref[0], live_ref[0], total_ref, so_far_ref
    )


def statistics(own, others, value, weight, live, me, group, lo, hi, so_far, index=None, slots=0):
    members = own.shape[1]
    parts = 1 + len(others)
    everyone = members * parts
    if index is None:
        width = math.gcd(math.gcd(lo, hi), 1024)
        lines = 0
        other_spec = pl.BlockSpec((1, members, width), lambda i, me: (0, 0, i))
    else:
        width = math.gcd(math.gcd(lo, hi), 512)
        lines = width // LANES
        other_spec = pl.BlockSpec(
            (members, width // slots * LANES), lambda i, me: (0, i)
        )
    skip = lo // width
    in_specs = [pl.BlockSpec((1, members, width), lambda i, me: (group, 0, skip + i))]
    in_specs += [other_spec] * len(others)
    in_specs += [pl.BlockSpec((1, 1, width), lambda i, me: (group, 0, skip + i))] * 3
    operands = [own, *others, value, weight, live]
    if index is not None:
        in_specs.append(pl.BlockSpec(index.shape, lambda i, me: (0, 0, 0)))
        operands.append(index)
    if so_far is not None:
        in_specs.append(pl.BlockSpec((everyone, LANES), lambda i, me: (0, 0)))
        operands.append(so_far)
    return pl.pallas_call(
        functools.partial(
            statistics_kernel, parts, slots, group, lo // LANES, lines, so_far is not None
        ),
        out_shape=jax.ShapeDtypeStruct((everyone, LANES), jnp.float32),
        grid_spec=pltpu.PrefetchScalarGridSpec(
            num_scalar_prefetch=1,
            grid=((hi - lo) // width,),
            in_specs=in_specs,
            out_specs=pl.BlockSpec((everyone, LANES), lambda i, me: (0, 0)),
            scratch_shapes=[pltpu.VMEM((everyone, width), jnp.float32)],
        ),
        compiler_params=pltpu.CompilerParams(dimension_semantics=("arbitrary",), vmem_limit_bytes=VMEM),
        name="statistics",
    )(me, *operands)


def transform_kernel(members, me_ref, stats_ref, transform_ref, mixer_ref, rest_ref):
    stats = stats_ref[...]
    everyone = stats.shape[0]
    gram = stats[:, :everyone]
    cross = stats[:, everyone : everyone + 1]
    misfit = stats[0:1, everyone + 1 : everyone + 2]
    total = stats[0:1, everyone + 2 : everyone + 3]
    dof = everyone - 1.0
    row = lax.broadcasted_iota(jnp.int32, (everyone, everyone), 0)
    col = lax.broadcasted_iota(jnp.int32, (everyone, everyone), 1)
    eye = (row == col).astype(jnp.float32)
    scl = dof / total
    gs = scl * gram
    bs = scl * cross
    qval = scl * misfit

    def whole_sum(x):
        return jnp.sum(jnp.sum(x, axis=1, keepdims=True), axis=0, keepdims=True)

    tval = whole_sum(gs * eye)
    rho = (1.0 + qval / dof) / (1.0 + tval / dof)
    amat = dof / rho * eye + gs
    scale = jnp.sqrt(whole_sum(amat * amat))

    def forward_step(_, carry):
        yn, zn = (split(x) for x in carry)
        tm = split(1.5 * eye - 0.5 * terms_dot(zn, yn))
        return terms_dot(yn, tm), terms_dot(tm, zn)

    yn = amat / scale
    tm = 1.5 * eye - 0.5 * yn
    yn, zn = lax.fori_loop(1, ITERS, forward_step, (terms_dot(split(yn), split(tm)), tm))
    parts = split(zn)
    pmat = terms_dot(parts, parts) / scale
    wide = jnp.broadcast_to(bs, (everyone, LANES))
    wbar = terms_dot(split(pmat), split(wide))[:, 0:1]
    transform = jnp.sqrt(dof) * zn / jnp.sqrt(scale) + wbar
    transform_ref[...] = transform
    held = pltpu.roll(transform, lax.rem(everyone - me_ref[0] * members, everyone), 0)
    mixer = held.T.astype(jnp.bfloat16)
    column_total = jnp.sum(mixer.astype(jnp.float32), axis=1, keepdims=True)
    extra = mixer_ref.shape[0] - everyone
    mixer_ref[...] = jnp.concatenate([mixer, jnp.ones((extra, everyone), jnp.bfloat16)], axis=0)
    rest_ref[...] = jnp.broadcast_to((1.0 - column_total) / everyone, rest_ref.shape)


def make_transform(stats, members, me):
    everyone = stats.shape[0]
    return pl.pallas_call(
        functools.partial(transform_kernel, members),
        out_shape=(
            jax.ShapeDtypeStruct((everyone, everyone), jnp.float32),
            jax.ShapeDtypeStruct((everyone + 16, everyone), jnp.bfloat16),
            jax.ShapeDtypeStruct((everyone, LANES), jnp.float32),
        ),
        in_specs=[pl.BlockSpec(memory_space=pltpu.SMEM), pl.BlockSpec(memory_space=pltpu.VMEM)],
        out_specs=(pl.BlockSpec(memory_space=pltpu.VMEM),) * 3,
        compiler_params=pltpu.CompilerParams(vmem_limit_bytes=VMEM),
        name="transform",
    )(me, stats)


def analysis_kernel(bounds, sources, aliased, base_ref, mixer_ref, rest_ref, own_ref, *refs):
    out_ref = refs[len(bounds) * sources + aliased]
    everyone, width = out_ref.shape
    members = own_ref.shape[0]
    step = pl.program_id(0)
    rest = rest_ref[:, 0:1]
    for i, (lo, hi) in enumerate(bounds):

        @pl.when((step >= lo) & (step < hi))
        def _(i=i, lo=lo):
            at = pl.ds(pl.multiple_of((step - lo) * width, width), width)
            cols = [own_ref[...]]
            cols += [ref[:, at] for ref in refs[i * sources : (i + 1) * sources]]
            if members % 16:
                cols = [x.astype(jnp.float32) for x in cols]
            cols = jnp.concatenate(cols, axis=0).astype(jnp.bfloat16)
            mixed = jnp.dot(mixer_ref[...], cols, preferred_element_type=jnp.float32)
            out = mixed[:everyone] + rest * mixed[everyone : everyone + 1]
            out_ref[...] = out.astype(out_ref.dtype)


def analyse(out, state, messages, mixer, rest, base, piece):
    members = state.shape[0]
    everyone = rest.shape[0]
    first, last = messages[0][0], messages[-1][1]
    width = piece // 4
    for lo, hi, _ in messages:
        width = math.gcd(width, lo, hi)
    skip = first // width
    whole = piece // width
    bounds = tuple((lo // width - skip, hi // width - skip) for lo, hi, _ in messages)
    received = [x for _, _, pieces in messages for x in pieces]
    aliased = int(out is not None)
    in_specs = [
        pl.BlockSpec(mixer.shape, lambda i, base: (0, 0)),
        pl.BlockSpec(rest.shape, lambda i, base: (0, 0)),
        pl.BlockSpec((members, width), lambda i, base: (0, base[0] * whole + skip + i)),
    ] + [pl.BlockSpec(memory_space=pltpu.VMEM)] * len(received)
    operands = [base, mixer, rest, state, *received]
    aliases = {}
    if aliased:
        in_specs.append(pl.BlockSpec(memory_space=pl.ANY))
        aliases = {len(operands): 0}
        operands.append(out)
    return pl.pallas_call(
        functools.partial(
            analysis_kernel, bounds, len(received) // len(messages), aliased
        ),
        out_shape=jax.ShapeDtypeStruct((everyone, piece), jnp.bfloat16),
        grid_spec=pltpu.PrefetchScalarGridSpec(
            num_scalar_prefetch=1,
            grid=((last - first) // width,),
            in_specs=in_specs,
            out_specs=pl.BlockSpec((everyone, width), lambda i, base: (0, skip + i)),
        ),
        input_output_aliases=aliases,
        compiler_params=pltpu.CompilerParams(
            dimension_semantics=("arbitrary",), vmem_limit_bytes=VMEM
        ),
        name="analysis",
    )(*operands)


def shards(state_a, state_b, obs_index, observation_count, obs_value, obs_weight):
    states = (state_a, state_b)
    members = state_a.shape[0]
    nmem = lax.axis_size("mem")
    ncol = lax.axis_size("col")
    piece = state_a.shape[1] // nmem
    nblk = obs_index.shape[1]
    slots = obs_index.shape[2]
    observations = nblk * slots
    unit = piece // 32
    me = lax.axis_index("mem")
    me_ref = me[None].astype(jnp.int32)
    shifts = range(1, nmem)

    def to_lower(array, shift):
        return lax.ppermute(array, "mem", [(i, (i - shift) % nmem) for i in range(nmem)])

    def to_upper(array, shift):
        return lax.ppermute(array, "mem", [(i, (i + shift) % nmem) for i in range(nmem)])

    def cut(message, source):
        group, lo, hi = message
        return [
            lax.dynamic_slice(
                source[group],
                (0, lax.rem(me + nmem - shift, nmem) * piece + lo * unit),
                (members, (hi - lo) * unit),
            )
            for shift in shifts
        ]

    others_index = [to_upper(obs_index, shift) for shift in shifts]
    index, *others_index = (
        x.reshape(2, observations // LANES, LANES) for x in (obs_index, *others_index)
    )

    group, lo, hi = MESSAGES[0]
    first_pieces = [
        cut_first(states[group], lax.rem(me_ref + nmem - shift, nmem), lo * unit, hi * unit, piece)
        for shift in shifts
    ]
    own_hx = gather(states, (0, 1), index, me_ref, slots, piece)
    sent_hx = [
        gather(states, SENT[:1], idx, lax.rem(me_ref + nmem - shift, nmem), slots, piece, SENT[1])
        for idx, shift in zip(others_index, shifts)
    ]
    got_hx = [to_lower(x, shift) for x, shift in zip(sent_hx, shifts)]

    live = (
        lax.broadcasted_iota(jnp.int32, (2, nblk, slots), 2) < observation_count[:, :, None]
    ).astype(jnp.float32)
    weight = (live * obs_weight).reshape(2, 1, observations)
    live = live.reshape(2, 1, observations)
    value = obs_value.reshape(2, 1, observations)

    received = {}

    def send(i, pieces):
        received[i] = [to_lower(x, shift) for x, shift in zip(pieces, shifts)]

    send(0, first_pieces)
    sources = lax.optimization_barrier((*states, sent_hx))
    for i, message in enumerate(MESSAGES[1:-1], 1):
        pieces = cut(message, sources)
        send(i, pieces)

    def read(i, so_far):
        group, lo, hi = MESSAGES[i]
        lo, hi = (x * observations // 32 for x in (lo, hi))
        return statistics(
            own_hx, received[i], value, weight, live, me_ref, group, lo, hi, so_far, index, slots
        )

    stats = read(READ[0], None)
    stats = statistics(
        own_hx,
        got_hx,
        value,
        weight,
        live,
        me_ref,
        SENT[0],
        SENT[1] * observations // 8,
        observations,
        stats,
    )
    for i in READ[1:]:
        stats = read(i, stats)

    pieces = cut(MESSAGES[-1], lax.optimization_barrier((*states, stats)))
    send(len(MESSAGES) - 1, pieces)

    def all_sum(x, axis, size):
        for i in range((size - 1).bit_length()):
            x = x + lax.ppermute(x, axis, [(j, j ^ (1 << i)) for j in range(size)])
        return x

    stats = all_sum(all_sum(stats, "mem", nmem), "col", ncol)
    transform, mixer, rest = make_transform(stats, members, me_ref)

    outs = [None, None]
    for call in CALLS:
        group = MESSAGES[call[0]][0]
        messages = [
            (MESSAGES[m][1] * unit, MESSAGES[m][2] * unit, received[m]) for m in call
        ]
        outs[group] = analyse(
            outs[group], states[group], messages, mixer, rest, me_ref, piece
        )
    return (outs[0], outs[1], transform)


def solution(mesh):
    return jax.shard_map(
        shards,
        mesh=mesh,
        in_specs=(
            P("mem", "col"),
            P("mem", "col"),
            P(None, ("col", "mem"), None),
            P(None, ("col", "mem")),
            P(None, ("col", "mem"), None),
            P(None, ("col", "mem"), None),
        ),
        out_specs=(P(None, ("col", "mem")), P(None, ("col", "mem")), P()),
        check_vma=False,
    )
```

```python
import functools
import math

import jax
import jax.numpy as jnp
from jax import lax
from jax.experimental import pallas as pl
from jax.experimental.pallas import tpu as pltpu
from jax.sharding import PartitionSpec as P


ITERS = 24
VMEM = 16 * 1024 * 1024
MOST_VMEM = 50 * 1024 * 1024
LANES = 128

MESSAGES = (
    (0, 0, 8),
    (0, 8, 16),
    (0, 16, 24),
    (0, 24, 32),
    (1, 0, 4),
    (1, 4, 6),
    (1, 6, 20),
    (1, 20, 28),
    (1, 28, 32),
)
READ = (0, 1, 2, 3, 4)
SENT = (1, 1)
CALLS = ((0, 1, 2, 3), (4, 5, 6), (7,), (8,))


def split(x):
    high = x.astype(jnp.bfloat16)
    rest = x - high.astype(jnp.float32)
    middle = rest.astype(jnp.bfloat16)
    return high, middle, (rest - middle.astype(jnp.float32)).astype(jnp.bfloat16)


def terms_dot(a, b):
    rows = a[0].shape[0]
    stacked = jnp.concatenate(a, axis=0)
    by_high = jnp.dot(stacked, b[0], preferred_element_type=jnp.float32)
    by_middle = jnp.dot(stacked[: 2 * rows], b[1], preferred_element_type=jnp.float32)
    by_low = jnp.dot(a[0], b[2], preferred_element_type=jnp.float32)
    second = by_high[rows : 2 * rows] + by_middle[:rows]
    third = by_high[2 * rows :] + by_middle[rows:] + by_low
    return by_high[:rows] + (second + third)


def cut_kernel(base_ref, state_ref, out_ref):
    out_ref[...] = state_ref[...]


def cut_first(state, base, lo, hi, piece):
    members, length = state.shape[0], hi - lo
    whole = piece // length
    return pl.pallas_call(
        cut_kernel,
        out_shape=jax.ShapeDtypeStruct((members, length), state.dtype),
        grid_spec=pltpu.PrefetchScalarGridSpec(
            num_scalar_prefetch=1,
            grid=(1,),
            in_specs=[
                pl.BlockSpec((members, length), lambda i, base: (0, base[0] * whole + lo // length))
            ],
            out_specs=pl.BlockSpec(memory_space=pltpu.VMEM),
        ),
        compiler_params=pltpu.CompilerParams(vmem_limit_bytes=MOST_VMEM),
        name="cut",
    )(base, state)


def take_rows(slots, ref, wanted_rows):
    per = LANES // slots
    rows = ref.shape[0]
    place = lax.broadcasted_iota(jnp.int32, (rows, LANES), 1) // slots
    for q, row in enumerate(wanted_rows):
        wanted = jnp.broadcast_to(row, (rows, LANES))
        acc = jnp.zeros((rows, LANES), jnp.float32)
        for j in range(per):
            start = (q * per + j) * LANES
            block = ref[:, start : start + LANES].astype(jnp.float32)
            taken = jnp.take_along_axis(block, wanted, axis=1, mode="promise_in_bounds")
            acc = jnp.where(place == j, taken, acc)
        yield q, acc


def gather_kernel(slots, groups, skip, base_ref, index_ref, *refs):
    out_ref = refs[-1]
    lines = out_ref.shape[2] // LANES
    first = (skip + pl.program_id(0)) * lines
    for i, group in enumerate(groups):
        rows = [index_ref[group, pl.ds(first + q, 1), :] for q in range(lines)]
        for q, taken in take_rows(slots, refs[i], rows):
            out_ref[i, :, q * LANES : (q + 1) * LANES] = taken.astype(out_ref.dtype)


def gather(states, groups, index, base, slots, piece, eighth=0):
    rows = states[0].shape[0]
    width = piece // 8
    steps = 8 - eighth
    observations = width // LANES * slots * steps
    state_spec = pl.BlockSpec((rows, width), lambda i, base: (0, base[0] * 8 + eighth + i))
    return pl.pallas_call(
        functools.partial(gather_kernel, slots, groups, eighth),
        out_shape=jax.ShapeDtypeStruct((len(groups), rows, observations), jnp.bfloat16),
        grid_spec=pltpu.PrefetchScalarGridSpec(
            num_scalar_prefetch=1,
            grid=(steps,),
            in_specs=[pl.BlockSpec(index.shape, lambda i, base: (0, 0, 0))]
            + [state_spec] * len(groups),
            out_specs=pl.BlockSpec(
                (len(groups), rows, observations // steps), lambda i, base: (0, 0, i)
            ),
        ),
        compiler_params=pltpu.CompilerParams(dimension_semantics=("arbitrary",), vmem_limit_bytes=VMEM),
        name="gather",
    )(base, index, *[states[group] for group in groups])


def add_statistics(hx, value, wt, live, total_ref, so_far_ref):
    everyone = hx.shape[0]
    hmean = jnp.sum(hx, axis=0, keepdims=True) / everyone
    anomaly = hx - hmean
    innov = value - hmean
    scaled = anomaly * wt
    product = lax.dot_general(
        jnp.concatenate(split(scaled), axis=0),
        jnp.concatenate(split(anomaly), axis=0),
        (((1,), (1,)), ((), ())),
        preferred_element_type=jnp.float32,
    )

    def term(i, j):
        rows = product[i * everyone : (i + 1) * everyone]
        return rows[:, j * everyone : (j + 1) * everyone]

    gram = term(0, 0) + (term(0, 1) + term(1, 0) + (term(0, 2) + term(2, 0) + term(1, 1)))
    cross = jnp.sum(scaled * innov, axis=1, keepdims=True)
    misfit = jnp.sum(wt * innov * innov, axis=1, keepdims=True)
    count = jnp.sum(live, axis=1, keepdims=True)
    lane = lax.broadcasted_iota(jnp.int32, (everyone, LANES - everyone), 1)
    side = jnp.where(lane == 0, cross, jnp.where(lane == 1, misfit, jnp.where(lane == 2, count, 0.0)))
    new = jnp.concatenate([gram, side], axis=1)

    @pl.when(pl.program_id(0) == 0)
    def _():
        total_ref[...] = new if so_far_ref is None else so_far_ref[...] + new

    @pl.when(pl.program_id(0) > 0)
    def _():
        total_ref[...] += new


def statistics_kernel(parts, slots, group, first, lines, started, me_ref, *refs):
    part_refs = refs[:parts]
    refs = refs[parts:]
    value_ref, weight_ref, live_ref = refs[:3]
    refs = refs[3:]
    index_ref = None
    if lines:
        index_ref, *refs = refs
    so_far_ref = None
    if started:
        so_far_ref, *refs = refs
    total_ref, all_ref = refs
    members = part_refs[0].shape[-2]
    me = me_ref[0]

    def place(j):
        return pl.ds(pl.multiple_of(lax.rem(me + j, parts) * members, members), members)

    all_ref[place(0), :] = part_refs[0][0].astype(jnp.float32)
    for j in range(1, parts):
        if not lines:
            all_ref[place(j), :] = part_refs[j][0].astype(jnp.float32)
            continue
        at = first + pl.program_id(0) * lines
        rows = [index_ref[group, pl.ds(at + q, 1), :] for q in range(lines)]
        for q, taken in take_rows(slots, part_refs[j], rows):
            all_ref[place(j), q * LANES : (q + 1) * LANES] = taken
    add_statistics(
        all_ref[...], value_ref[0], weight_ref[0], live_ref[0], total_ref, so_far_ref
    )


def statistics(own, others, value, weight, live, me, group, lo, hi, so_far, index=None, slots=0):
    members = own.shape[1]
    parts = 1 + len(others)
    everyone = members * parts
    if index is None:
        width = math.gcd(math.gcd(lo, hi), 1024)
        lines = 0
        other_spec = pl.BlockSpec((1, members, width), lambda i, me: (0, 0, i))
    else:
        width = math.gcd(math.gcd(lo, hi), 512)
        lines = width // LANES
        other_spec = pl.BlockSpec(
            (members, width // slots * LANES), lambda i, me: (0, i)
        )
    skip = lo // width
    in_specs = [pl.BlockSpec((1, members, width), lambda i, me: (group, 0, skip + i))]
    in_specs += [other_spec] * len(others)
    in_specs += [pl.BlockSpec((1, 1, width), lambda i, me: (group, 0, skip + i))] * 3
    operands = [own, *others, value, weight, live]
    if index is not None:
        in_specs.append(pl.BlockSpec(index.shape, lambda i, me: (0, 0, 0)))
        operands.append(index)
    if so_far is not None:
        in_specs.append(pl.BlockSpec((everyone, LANES), lambda i, me: (0, 0)))
        operands.append(so_far)
    return pl.pallas_call(
        functools.partial(
            statistics_kernel, parts, slots, group, lo // LANES, lines, so_far is not None
        ),
        out_shape=jax.ShapeDtypeStruct((everyone, LANES), jnp.float32),
        grid_spec=pltpu.PrefetchScalarGridSpec(
            num_scalar_prefetch=1,
            grid=((hi - lo) // width,),
            in_specs=in_specs,
            out_specs=pl.BlockSpec((everyone, LANES), lambda i, me: (0, 0)),
            scratch_shapes=[pltpu.VMEM((everyone, width), jnp.float32)],
        ),
        compiler_params=pltpu.CompilerParams(dimension_semantics=("arbitrary",), vmem_limit_bytes=VMEM),
        name="statistics",
    )(me, *operands)


def transform_kernel(members, me_ref, stats_ref, transform_ref, mixer_ref, rest_ref):
    stats = stats_ref[...]
    everyone = stats.shape[0]
    gram = stats[:, :everyone]
    cross = stats[:, everyone : everyone + 1]
    misfit = stats[0:1, everyone + 1 : everyone + 2]
    total = stats[0:1, everyone + 2 : everyone + 3]
    dof = everyone - 1.0
    row = lax.broadcasted_iota(jnp.int32, (everyone, everyone), 0)
    col = lax.broadcasted_iota(jnp.int32, (everyone, everyone), 1)
    eye = (row == col).astype(jnp.float32)
    scl = dof / total
    gs = scl * gram
    bs = scl * cross
    qval = scl * misfit

    def whole_sum(x):
        return jnp.sum(jnp.sum(x, axis=1, keepdims=True), axis=0, keepdims=True)

    tval = whole_sum(gs * eye)
    rho = (1.0 + qval / dof) / (1.0 + tval / dof)
    amat = dof / rho * eye + gs
    scale = jnp.sqrt(whole_sum(amat * amat))

    def forward_step(_, carry):
        yn, zn = (split(x) for x in carry)
        tm = split(1.5 * eye - 0.5 * terms_dot(zn, yn))
        return terms_dot(yn, tm), terms_dot(tm, zn)

    yn = amat / scale
    tm = 1.5 * eye - 0.5 * yn
    yn, zn = lax.fori_loop(1, ITERS, forward_step, (terms_dot(split(yn), split(tm)), tm))
    parts = split(zn)
    pmat = terms_dot(parts, parts) / scale
    wide = jnp.broadcast_to(bs, (everyone, LANES))
    wbar = terms_dot(split(pmat), split(wide))[:, 0:1]
    transform = jnp.sqrt(dof) * zn / jnp.sqrt(scale) + wbar
    transform_ref[...] = transform
    held = pltpu.roll(transform, lax.rem(everyone - me_ref[0] * members, everyone), 0)
    mixer = held.T.astype(jnp.bfloat16)
    column_total = jnp.sum(mixer.astype(jnp.float32), axis=1, keepdims=True)
    extra = mixer_ref.shape[0] - everyone
    mixer_ref[...] = jnp.concatenate([mixer, jnp.ones((extra, everyone), jnp.bfloat16)], axis=0)
    rest_ref[...] = jnp.broadcast_to((1.0 - column_total) / everyone, rest_ref.shape)


def make_transform(stats, members, me):
    everyone = stats.shape[0]
    return pl.pallas_call(
        functools.partial(transform_kernel, members),
        out_shape=(
            jax.ShapeDtypeStruct((everyone, everyone), jnp.float32),
            jax.ShapeDtypeStruct((everyone + 16, everyone), jnp.bfloat16),
            jax.ShapeDtypeStruct((everyone, LANES), jnp.float32),
        ),
        in_specs=[pl.BlockSpec(memory_space=pltpu.SMEM), pl.BlockSpec(memory_space=pltpu.VMEM)],
        out_specs=(pl.BlockSpec(memory_space=pltpu.VMEM),) * 3,
        compiler_params=pltpu.CompilerParams(vmem_limit_bytes=VMEM),
        name="transform",
    )(me, stats)


def step_pieces(bounds, start, end):
    pieces = []
    for i, (lo, hi) in enumerate(bounds):
        if lo < end and start < hi:
            pieces.append((i, max(lo, start) - lo, min(hi, end) - lo))
    return pieces


def analysis_kernel(bounds, sources, skip, aliased, base_ref, mixer_ref, rest_ref, own_ref, *refs):
    out_ref = refs[len(bounds) * sources + aliased]
    everyone, width = out_ref.shape
    members = own_ref.shape[0]
    rest = rest_ref[:, 0:1]
    for step in range((bounds[-1][1] - bounds[0][0]) // width):

        @pl.when(pl.program_id(0) == step)
        def _(step=step):
            start = (skip + step) * width
            pieces = step_pieces(bounds, start, start + width)
            cols = [own_ref[...]]
            for source in range(sources):
                parts = [refs[i * sources + source][:, lo:hi] for i, lo, hi in pieces]
                cols.append(parts[0] if len(parts) == 1 else jnp.concatenate(parts, axis=1))
            if members % 16:
                cols = [x.astype(jnp.float32) for x in cols]
            cols = jnp.concatenate(cols, axis=0).astype(jnp.bfloat16)
            mixed = jnp.dot(mixer_ref[...], cols, preferred_element_type=jnp.float32)
            out = mixed[:everyone] + rest * mixed[everyone : everyone + 1]
            out_ref[...] = out.astype(out_ref.dtype)


def analyse(out, state, messages, mixer, rest, base, piece):
    members = state.shape[0]
    everyone = rest.shape[0]
    bounds = tuple((lo, hi) for lo, hi, _ in messages)
    first, last = bounds[0][0], bounds[-1][1]
    width = math.gcd(piece // 4, first, last)
    skip = first // width
    whole = piece // width
    received = [x for _, _, pieces in messages for x in pieces]
    aliased = int(out is not None)
    in_specs = [
        pl.BlockSpec(mixer.shape, lambda i, base: (0, 0)),
        pl.BlockSpec(rest.shape, lambda i, base: (0, 0)),
        pl.BlockSpec((members, width), lambda i, base: (0, base[0] * whole + skip + i)),
    ] + [pl.BlockSpec(memory_space=pltpu.VMEM)] * len(received)
    operands = [base, mixer, rest, state, *received]
    aliases = {}
    if aliased:
        in_specs.append(pl.BlockSpec(memory_space=pl.ANY))
        aliases = {len(operands): 0}
        operands.append(out)
    return pl.pallas_call(
        functools.partial(
            analysis_kernel, bounds, len(received) // len(messages), skip, aliased
        ),
        out_shape=jax.ShapeDtypeStruct((everyone, piece), jnp.bfloat16),
        grid_spec=pltpu.PrefetchScalarGridSpec(
            num_scalar_prefetch=1,
            grid=((last - first) // width,),
            in_specs=in_specs,
            out_specs=pl.BlockSpec((everyone, width), lambda i, base: (0, skip + i)),
        ),
        input_output_aliases=aliases,
        compiler_params=pltpu.CompilerParams(
            dimension_semantics=("arbitrary",), vmem_limit_bytes=VMEM
        ),
        name="analysis",
    )(*operands)


def shards(state_a, state_b, obs_index, observation_count, obs_value, obs_weight):
    states = (state_a, state_b)
    members = state_a.shape[0]
    nmem = lax.axis_size("mem")
    ncol = lax.axis_size("col")
    piece = state_a.shape[1] // nmem
    nblk = obs_index.shape[1]
    slots = obs_index.shape[2]
    observations = nblk * slots
    unit = piece // 32
    me = lax.axis_index("mem")
    me_ref = me[None].astype(jnp.int32)
    shifts = range(1, nmem)

    def to_lower(array, shift):
        return lax.ppermute(array, "mem", [(i, (i - shift) % nmem) for i in range(nmem)])

    def to_upper(array, shift):
        return lax.ppermute(array, "mem", [(i, (i + shift) % nmem) for i in range(nmem)])

    def cut(message, source):
        group, lo, hi = message
        return [
            lax.dynamic_slice(
                source[group],
                (0, lax.rem(me + nmem - shift, nmem) * piece + lo * unit),
                (members, (hi - lo) * unit),
            )
            for shift in shifts
        ]

    others_index = [to_upper(obs_index, shift) for shift in shifts]
    index, *others_index = (
        x.reshape(2, observations // LANES, LANES) for x in (obs_index, *others_index)
    )

    group, lo, hi = MESSAGES[0]
    first_pieces = [
        cut_first(states[group], lax.rem(me_ref + nmem - shift, nmem), lo * unit, hi * unit, piece)
        for shift in shifts
    ]
    own_hx = gather(states, (0, 1), index, me_ref, slots, piece)
    sent_hx = [
        gather(states, SENT[:1], idx, lax.rem(me_ref + nmem - shift, nmem), slots, piece, SENT[1])
        for idx, shift in zip(others_index, shifts)
    ]
    got_hx = [to_lower(x, shift) for x, shift in zip(sent_hx, shifts)]

    live = (
        lax.broadcasted_iota(jnp.int32, (2, nblk, slots), 2) < observation_count[:, :, None]
    ).astype(jnp.float32)
    weight = (live * obs_weight).reshape(2, 1, observations)
    live = live.reshape(2, 1, observations)
    value = obs_value.reshape(2, 1, observations)

    received = {}

    def send(i, pieces):
        received[i] = [to_lower(x, shift) for x, shift in zip(pieces, shifts)]

    send(0, first_pieces)
    sources = lax.optimization_barrier((*states, sent_hx))
    for i, message in enumerate(MESSAGES[1:-1], 1):
        pieces = cut(message, sources)
        send(i, pieces)

    def read(i, so_far):
        group, lo, hi = MESSAGES[i]
        lo, hi = (x * observations // 32 for x in (lo, hi))
        return statistics(
            own_hx, received[i], value, weight, live, me_ref, group, lo, hi, so_far, index, slots
        )

    stats = read(READ[0], None)
    stats = statistics(
        own_hx,
        got_hx,
        value,
        weight,
        live,
        me_ref,
        SENT[0],
        SENT[1] * observations // 8,
        observations,
        stats,
    )
    for i in READ[1:]:
        stats = read(i, stats)

    pieces = cut(MESSAGES[-1], lax.optimization_barrier((*states, stats)))
    send(len(MESSAGES) - 1, pieces)

    def all_sum(x, axis, size):
        for i in range((size - 1).bit_length()):
            x = x + lax.ppermute(x, axis, [(j, j ^ (1 << i)) for j in range(size)])
        return x

    stats = all_sum(all_sum(stats, "mem", nmem), "col", ncol)
    transform, mixer, rest = make_transform(stats, members, me_ref)

    outs = [None, None]
    for call in CALLS:
        group = MESSAGES[call[0]][0]
        messages = [
            (MESSAGES[m][1] * unit, MESSAGES[m][2] * unit, received[m]) for m in call
        ]
        outs[group] = analyse(
            outs[group], states[group], messages, mixer, rest, me_ref, piece
        )
    return (outs[0], outs[1], transform)


def solution(mesh):
    return jax.shard_map(
        shards,
        mesh=mesh,
        in_specs=(
            P("mem", "col"),
            P("mem", "col"),
            P(None, ("col", "mem"), None),
            P(None, ("col", "mem")),
            P(None, ("col", "mem"), None),
            P(None, ("col", "mem"), None),
        ),
        out_specs=(P(None, ("col", "mem")), P(None, ("col", "mem")), P()),
        check_vma=False,
    )
```

```python
import functools
import math

import jax
import jax.numpy as jnp
from jax import lax
from jax.experimental import pallas as pl
from jax.experimental.pallas import tpu as pltpu
from jax.sharding import PartitionSpec as P


ITERS = 24
VMEM = 16 * 1024 * 1024
MOST_VMEM = 50 * 1024 * 1024
LANES = 128

MESSAGES = (
    (0, 0, 8),
    (0, 8, 32),
    (1, 0, 4),
    (1, 4, 6),
    (1, 6, 20),
    (1, 20, 28),
    (1, 28, 32),
)
READ = (0, 1, 2)
SENT = (1, 1)
CALLS = ((0, 1), (2, 3, 4), (5,), (6,))


def split(x):
    high = x.astype(jnp.bfloat16)
    rest = x - high.astype(jnp.float32)
    middle = rest.astype(jnp.bfloat16)
    return high, middle, (rest - middle.astype(jnp.float32)).astype(jnp.bfloat16)


def terms_dot(a, b):
    rows = a[0].shape[0]
    stacked = jnp.concatenate(a, axis=0)
    by_high = jnp.dot(stacked, b[0], preferred_element_type=jnp.float32)
    by_middle = jnp.dot(stacked[: 2 * rows], b[1], preferred_element_type=jnp.float32)
    by_low = jnp.dot(a[0], b[2], preferred_element_type=jnp.float32)
    second = by_high[rows : 2 * rows] + by_middle[:rows]
    third = by_high[2 * rows :] + by_middle[rows:] + by_low
    return by_high[:rows] + (second + third)


def cut_kernel(base_ref, state_ref, out_ref):
    out_ref[...] = state_ref[...]


def cut_first(state, base, lo, hi, piece):
    members, length = state.shape[0], hi - lo
    whole = piece // length
    return pl.pallas_call(
        cut_kernel,
        out_shape=jax.ShapeDtypeStruct((members, length), state.dtype),
        grid_spec=pltpu.PrefetchScalarGridSpec(
            num_scalar_prefetch=1,
            grid=(1,),
            in_specs=[
                pl.BlockSpec((members, length), lambda i, base: (0, base[0] * whole + lo // length))
            ],
            out_specs=pl.BlockSpec(memory_space=pltpu.VMEM),
        ),
        compiler_params=pltpu.CompilerParams(vmem_limit_bytes=MOST_VMEM),
        name="cut",
    )(base, state)


def take_rows(slots, ref, wanted_rows):
    per = LANES // slots
    rows = ref.shape[0]
    place = lax.broadcasted_iota(jnp.int32, (rows, LANES), 1) // slots
    for q, row in enumerate(wanted_rows):
        wanted = jnp.broadcast_to(row, (rows, LANES))
        acc = jnp.zeros((rows, LANES), jnp.float32)
        for j in range(per):
            start = (q * per + j) * LANES
            block = ref[:, start : start + LANES].astype(jnp.float32)
            taken = jnp.take_along_axis(block, wanted, axis=1, mode="promise_in_bounds")
            acc = jnp.where(place == j, taken, acc)
        yield q, acc


def gather_kernel(slots, groups, skip, base_ref, index_ref, *refs):
    out_ref = refs[-1]
    lines = out_ref.shape[2] // LANES
    first = (skip + pl.program_id(0)) * lines
    for i, group in enumerate(groups):
        rows = [index_ref[group, pl.ds(first + q, 1), :] for q in range(lines)]
        for q, taken in take_rows(slots, refs[i], rows):
            out_ref[i, :, q * LANES : (q + 1) * LANES] = taken.astype(out_ref.dtype)


def gather(states, groups, index, base, slots, piece, eighth=0):
    rows = states[0].shape[0]
    width = piece // 8
    steps = 8 - eighth
    observations = width // LANES * slots * steps
    state_spec = pl.BlockSpec((rows, width), lambda i, base: (0, base[0] * 8 + eighth + i))
    return pl.pallas_call(
        functools.partial(gather_kernel, slots, groups, eighth),
        out_shape=jax.ShapeDtypeStruct((len(groups), rows, observations), jnp.bfloat16),
        grid_spec=pltpu.PrefetchScalarGridSpec(
            num_scalar_prefetch=1,
            grid=(steps,),
            in_specs=[pl.BlockSpec(index.shape, lambda i, base: (0, 0, 0))]
            + [state_spec] * len(groups),
            out_specs=pl.BlockSpec(
                (len(groups), rows, observations // steps), lambda i, base: (0, 0, i)
            ),
        ),
        compiler_params=pltpu.CompilerParams(dimension_semantics=("arbitrary",), vmem_limit_bytes=VMEM),
        name="gather",
    )(base, index, *[states[group] for group in groups])


def add_statistics(hx, value, wt, live, total_ref, so_far_ref):
    everyone = hx.shape[0]
    hmean = jnp.sum(hx, axis=0, keepdims=True) / everyone
    anomaly = hx - hmean
    innov = value - hmean
    scaled = anomaly * wt
    product = lax.dot_general(
        jnp.concatenate(split(scaled), axis=0),
        jnp.concatenate(split(anomaly), axis=0),
        (((1,), (1,)), ((), ())),
        preferred_element_type=jnp.float32,
    )

    def term(i, j):
        rows = product[i * everyone : (i + 1) * everyone]
        return rows[:, j * everyone : (j + 1) * everyone]

    gram = term(0, 0) + (term(0, 1) + term(1, 0) + (term(0, 2) + term(2, 0) + term(1, 1)))
    cross = jnp.sum(scaled * innov, axis=1, keepdims=True)
    misfit = jnp.sum(wt * innov * innov, axis=1, keepdims=True)
    count = jnp.sum(live, axis=1, keepdims=True)
    lane = lax.broadcasted_iota(jnp.int32, (everyone, LANES - everyone), 1)
    side = jnp.where(lane == 0, cross, jnp.where(lane == 1, misfit, jnp.where(lane == 2, count, 0.0)))
    new = jnp.concatenate([gram, side], axis=1)

    @pl.when(pl.program_id(0) == 0)
    def _():
        total_ref[...] = new if so_far_ref is None else so_far_ref[...] + new

    @pl.when(pl.program_id(0) > 0)
    def _():
        total_ref[...] += new


def statistics_kernel(parts, slots, group, first, lines, started, me_ref, *refs):
    part_refs = refs[:parts]
    refs = refs[parts:]
    value_ref, weight_ref, live_ref = refs[:3]
    refs = refs[3:]
    index_ref = None
    if lines:
        index_ref, *refs = refs
    so_far_ref = None
    if started:
        so_far_ref, *refs = refs
    total_ref, all_ref = refs
    members = part_refs[0].shape[-2]
    me = me_ref[0]

    def place(j):
        return pl.ds(pl.multiple_of(lax.rem(me + j, parts) * members, members), members)

    all_ref[place(0), :] = part_refs[0][0].astype(jnp.float32)
    for j in range(1, parts):
        if not lines:
            all_ref[place(j), :] = part_refs[j][0].astype(jnp.float32)
            continue
        at = first + pl.program_id(0) * lines
        rows = [index_ref[group, pl.ds(at + q, 1), :] for q in range(lines)]
        for q, taken in take_rows(slots, part_refs[j], rows):
            all_ref[place(j), q * LANES : (q + 1) * LANES] = taken
    add_statistics(
        all_ref[...], value_ref[0], weight_ref[0], live_ref[0], total_ref, so_far_ref
    )


def statistics(own, others, value, weight, live, me, group, lo, hi, so_far, index=None, slots=0):
    members = own.shape[1]
    parts = 1 + len(others)
    everyone = members * parts
    if index is None:
        width = math.gcd(math.gcd(lo, hi), 1024)
        lines = 0
        other_spec = pl.BlockSpec((1, members, width), lambda i, me: (0, 0, i))
    else:
        width = math.gcd(math.gcd(lo, hi), 512)
        lines = width // LANES
        other_spec = pl.BlockSpec(
            (members, width // slots * LANES), lambda i, me: (0, i)
        )
    skip = lo // width
    in_specs = [pl.BlockSpec((1, members, width), lambda i, me: (group, 0, skip + i))]
    in_specs += [other_spec] * len(others)
    in_specs += [pl.BlockSpec((1, 1, width), lambda i, me: (group, 0, skip + i))] * 3
    operands = [own, *others, value, weight, live]
    if index is not None:
        in_specs.append(pl.BlockSpec(index.shape, lambda i, me: (0, 0, 0)))
        operands.append(index)
    if so_far is not None:
        in_specs.append(pl.BlockSpec((everyone, LANES), lambda i, me: (0, 0)))
        operands.append(so_far)
    return pl.pallas_call(
        functools.partial(
            statistics_kernel, parts, slots, group, lo // LANES, lines, so_far is not None
        ),
        out_shape=jax.ShapeDtypeStruct((everyone, LANES), jnp.float32),
        grid_spec=pltpu.PrefetchScalarGridSpec(
            num_scalar_prefetch=1,
            grid=((hi - lo) // width,),
            in_specs=in_specs,
            out_specs=pl.BlockSpec((everyone, LANES), lambda i, me: (0, 0)),
            scratch_shapes=[pltpu.VMEM((everyone, width), jnp.float32)],
        ),
        compiler_params=pltpu.CompilerParams(dimension_semantics=("arbitrary",), vmem_limit_bytes=VMEM),
        name="statistics",
    )(me, *operands)


def transform_kernel(members, me_ref, stats_ref, transform_ref, mixer_ref, rest_ref):
    stats = stats_ref[...]
    everyone = stats.shape[0]
    gram = stats[:, :everyone]
    cross = stats[:, everyone : everyone + 1]
    misfit = stats[0:1, everyone + 1 : everyone + 2]
    total = stats[0:1, everyone + 2 : everyone + 3]
    dof = everyone - 1.0
    row = lax.broadcasted_iota(jnp.int32, (everyone, everyone), 0)
    col = lax.broadcasted_iota(jnp.int32, (everyone, everyone), 1)
    eye = (row == col).astype(jnp.float32)
    scl = dof / total
    gs = scl * gram
    bs = scl * cross
    qval = scl * misfit

    def whole_sum(x):
        return jnp.sum(jnp.sum(x, axis=1, keepdims=True), axis=0, keepdims=True)

    tval = whole_sum(gs * eye)
    rho = (1.0 + qval / dof) / (1.0 + tval / dof)
    amat = dof / rho * eye + gs
    scale = jnp.sqrt(whole_sum(amat * amat))

    def forward_step(_, carry):
        yn, zn = (split(x) for x in carry)
        tm = split(1.5 * eye - 0.5 * terms_dot(zn, yn))
        return terms_dot(yn, tm), terms_dot(tm, zn)

    yn = amat / scale
    tm = 1.5 * eye - 0.5 * yn
    yn, zn = lax.fori_loop(1, ITERS, forward_step, (terms_dot(split(yn), split(tm)), tm))
    parts = split(zn)
    pmat = terms_dot(parts, parts) / scale
    wide = jnp.broadcast_to(bs, (everyone, LANES))
    wbar = terms_dot(split(pmat), split(wide))[:, 0:1]
    transform = jnp.sqrt(dof) * zn / jnp.sqrt(scale) + wbar
    transform_ref[...] = transform
    held = pltpu.roll(transform, lax.rem(everyone - me_ref[0] * members, everyone), 0)
    mixer = held.T.astype(jnp.bfloat16)
    column_total = jnp.sum(mixer.astype(jnp.float32), axis=1, keepdims=True)
    extra = mixer_ref.shape[0] - everyone
    mixer_ref[...] = jnp.concatenate([mixer, jnp.ones((extra, everyone), jnp.bfloat16)], axis=0)
    rest_ref[...] = jnp.broadcast_to((1.0 - column_total) / everyone, rest_ref.shape)


def make_transform(stats, members, me):
    everyone = stats.shape[0]
    return pl.pallas_call(
        functools.partial(transform_kernel, members),
        out_shape=(
            jax.ShapeDtypeStruct((everyone, everyone), jnp.float32),
            jax.ShapeDtypeStruct((everyone + 16, everyone), jnp.bfloat16),
            jax.ShapeDtypeStruct((everyone, LANES), jnp.float32),
        ),
        in_specs=[pl.BlockSpec(memory_space=pltpu.SMEM), pl.BlockSpec(memory_space=pltpu.VMEM)],
        out_specs=(pl.BlockSpec(memory_space=pltpu.VMEM),) * 3,
        compiler_params=pltpu.CompilerParams(vmem_limit_bytes=VMEM),
        name="transform",
    )(me, stats)


def step_pieces(bounds, start, end):
    pieces = []
    for i, (lo, hi) in enumerate(bounds):
        if lo < end and start < hi:
            pieces.append((i, max(lo, start) - lo, min(hi, end) - lo))
    return pieces


def analysis_kernel(bounds, sources, skip, aliased, base_ref, mixer_ref, rest_ref, own_ref, *refs):
    out_ref = refs[len(bounds) * sources + aliased]
    everyone, width = out_ref.shape
    members = own_ref.shape[0]
    rest = rest_ref[:, 0:1]
    for step in range((bounds[-1][1] - bounds[0][0]) // width):

        @pl.when(pl.program_id(0) == step)
        def _(step=step):
            start = (skip + step) * width
            pieces = step_pieces(bounds, start, start + width)
            cols = [own_ref[...]]
            for source in range(sources):
                parts = [refs[i * sources + source][:, lo:hi] for i, lo, hi in pieces]
                cols.append(parts[0] if len(parts) == 1 else jnp.concatenate(parts, axis=1))
            if members % 16:
                cols = [x.astype(jnp.float32) for x in cols]
            cols = jnp.concatenate(cols, axis=0).astype(jnp.bfloat16)
            mixed = jnp.dot(mixer_ref[...], cols, preferred_element_type=jnp.float32)
            out = mixed[:everyone] + rest * mixed[everyone : everyone + 1]
            out_ref[...] = out.astype(out_ref.dtype)


def analyse(out, state, messages, mixer, rest, base, piece):
    members = state.shape[0]
    everyone = rest.shape[0]
    bounds = tuple((lo, hi) for lo, hi, _ in messages)
    first, last = bounds[0][0], bounds[-1][1]
    width = math.gcd(piece // 4, first, last)
    skip = first // width
    whole = piece // width
    received = [x for _, _, pieces in messages for x in pieces]
    aliased = int(out is not None)
    in_specs = [
        pl.BlockSpec(mixer.shape, lambda i, base: (0, 0)),
        pl.BlockSpec(rest.shape, lambda i, base: (0, 0)),
        pl.BlockSpec((members, width), lambda i, base: (0, base[0] * whole + skip + i)),
    ] + [pl.BlockSpec(memory_space=pltpu.VMEM)] * len(received)
    operands = [base, mixer, rest, state, *received]
    aliases = {}
    if aliased:
        in_specs.append(pl.BlockSpec(memory_space=pl.ANY))
        aliases = {len(operands): 0}
        operands.append(out)
    return pl.pallas_call(
        functools.partial(
            analysis_kernel, bounds, len(received) // len(messages), skip, aliased
        ),
        out_shape=jax.ShapeDtypeStruct((everyone, piece), jnp.bfloat16),
        grid_spec=pltpu.PrefetchScalarGridSpec(
            num_scalar_prefetch=1,
            grid=((last - first) // width,),
            in_specs=in_specs,
            out_specs=pl.BlockSpec((everyone, width), lambda i, base: (0, skip + i)),
        ),
        input_output_aliases=aliases,
        compiler_params=pltpu.CompilerParams(
            dimension_semantics=("arbitrary",), vmem_limit_bytes=VMEM
        ),
        name="analysis",
    )(*operands)


def shards(state_a, state_b, obs_index, observation_count, obs_value, obs_weight):
    states = (state_a, state_b)
    members = state_a.shape[0]
    nmem = lax.axis_size("mem")
    ncol = lax.axis_size("col")
    piece = state_a.shape[1] // nmem
    nblk = obs_index.shape[1]
    slots = obs_index.shape[2]
    observations = nblk * slots
    unit = piece // 32
    me = lax.axis_index("mem")
    me_ref = me[None].astype(jnp.int32)
    shifts = range(1, nmem)

    def to_lower(array, shift):
        return lax.ppermute(array, "mem", [(i, (i - shift) % nmem) for i in range(nmem)])

    def to_upper(array, shift):
        return lax.ppermute(array, "mem", [(i, (i + shift) % nmem) for i in range(nmem)])

    def cut(message, source):
        group, lo, hi = message
        return [
            lax.dynamic_slice(
                source[group],
                (0, lax.rem(me + nmem - shift, nmem) * piece + lo * unit),
                (members, (hi - lo) * unit),
            )
            for shift in shifts
        ]

    others_index = [to_upper(obs_index, shift) for shift in shifts]
    index, *others_index = (
        x.reshape(2, observations // LANES, LANES) for x in (obs_index, *others_index)
    )

    group, lo, hi = MESSAGES[0]
    first_pieces = [
        cut_first(states[group], lax.rem(me_ref + nmem - shift, nmem), lo * unit, hi * unit, piece)
        for shift in shifts
    ]
    own_hx = gather(states, (0, 1), index, me_ref, slots, piece)
    sent_hx = [
        gather(states, SENT[:1], idx, lax.rem(me_ref + nmem - shift, nmem), slots, piece, SENT[1])
        for idx, shift in zip(others_index, shifts)
    ]
    got_hx = [to_lower(x, shift) for x, shift in zip(sent_hx, shifts)]

    live = (
        lax.broadcasted_iota(jnp.int32, (2, nblk, slots), 2) < observation_count[:, :, None]
    ).astype(jnp.float32)
    weight = (live * obs_weight).reshape(2, 1, observations)
    live = live.reshape(2, 1, observations)
    value = obs_value.reshape(2, 1, observations)

    received = {}

    def send(i, pieces):
        received[i] = [to_lower(x, shift) for x, shift in zip(pieces, shifts)]

    send(0, first_pieces)
    sources = lax.optimization_barrier((*states, sent_hx))
    for i, message in enumerate(MESSAGES[1:-1], 1):
        pieces = cut(message, sources)
        send(i, pieces)

    def read(i, so_far):
        group, lo, hi = MESSAGES[i]
        lo, hi = (x * observations // 32 for x in (lo, hi))
        return statistics(
            own_hx, received[i], value, weight, live, me_ref, group, lo, hi, so_far, index, slots
        )

    stats = read(READ[0], None)
    stats = statistics(
        own_hx,
        got_hx,
        value,
        weight,
        live,
        me_ref,
        SENT[0],
        SENT[1] * observations // 8,
        observations,
        stats,
    )
    for i in READ[1:]:
        stats = read(i, stats)

    pieces = cut(MESSAGES[-1], lax.optimization_barrier((*states, stats)))
    send(len(MESSAGES) - 1, pieces)

    def all_sum(x, axis, size):
        for i in range((size - 1).bit_length()):
            x = x + lax.ppermute(x, axis, [(j, j ^ (1 << i)) for j in range(size)])
        return x

    stats = all_sum(all_sum(stats, "mem", nmem), "col", ncol)
    transform, mixer, rest = make_transform(stats, members, me_ref)

    outs = [None, None]
    for call in CALLS:
        group = MESSAGES[call[0]][0]
        messages = [
            (MESSAGES[m][1] * unit, MESSAGES[m][2] * unit, received[m]) for m in call
        ]
        outs[group] = analyse(
            outs[group], states[group], messages, mixer, rest, me_ref, piece
        )
    return (outs[0], outs[1], transform)


def solution(mesh):
    return jax.shard_map(
        shards,
        mesh=mesh,
        in_specs=(
            P("mem", "col"),
            P("mem", "col"),
            P(None, ("col", "mem"), None),
            P(None, ("col", "mem")),
            P(None, ("col", "mem"), None),
            P(None, ("col", "mem"), None),
        ),
        out_specs=(P(None, ("col", "mem")), P(None, ("col", "mem")), P()),
        check_vma=False,
    )
```

```python
import functools
import math

import jax
import jax.numpy as jnp
from jax import lax
from jax.experimental import pallas as pl
from jax.experimental.pallas import tpu as pltpu
from jax.sharding import PartitionSpec as P


ITERS = 24
VMEM = 16 * 1024 * 1024
MOST_VMEM = 50 * 1024 * 1024
LANES = 128

MESSAGES = (
    (0, 0, 8),
    (0, 8, 32),
    (1, 0, 4),
    (1, 4, 6),
    (1, 6, 20),
    (1, 20, 30),
    (1, 30, 32),
)
READ = (0, 1, 2)
SENT = (1, 1)
CALLS = ((0, 1), (2, 3, 4), (5,), (6,))


def split(x):
    high = x.astype(jnp.bfloat16)
    rest = x - high.astype(jnp.float32)
    middle = rest.astype(jnp.bfloat16)
    return high, middle, (rest - middle.astype(jnp.float32)).astype(jnp.bfloat16)


def terms_dot(a, b):
    rows = a[0].shape[0]
    stacked = jnp.concatenate(a, axis=0)
    by_high = jnp.dot(stacked, b[0], preferred_element_type=jnp.float32)
    by_middle = jnp.dot(stacked[: 2 * rows], b[1], preferred_element_type=jnp.float32)
    by_low = jnp.dot(a[0], b[2], preferred_element_type=jnp.float32)
    second = by_high[rows : 2 * rows] + by_middle[:rows]
    third = by_high[2 * rows :] + by_middle[rows:] + by_low
    return by_high[:rows] + (second + third)


def cut_kernel(base_ref, state_ref, out_ref):
    out_ref[...] = state_ref[...]


def cut_out(state, base, lo, hi, piece, vmem):
    members, length = state.shape[0], hi - lo
    whole = piece // length
    return pl.pallas_call(
        cut_kernel,
        out_shape=jax.ShapeDtypeStruct((members, length), state.dtype),
        grid_spec=pltpu.PrefetchScalarGridSpec(
            num_scalar_prefetch=1,
            grid=(1,),
            in_specs=[
                pl.BlockSpec((members, length), lambda i, base: (0, base[0] * whole + lo // length))
            ],
            out_specs=pl.BlockSpec(memory_space=pltpu.VMEM),
        ),
        compiler_params=pltpu.CompilerParams(vmem_limit_bytes=vmem),
        name="cut",
    )(base, state)


def take_rows(slots, ref, wanted_rows):
    per = LANES // slots
    rows = ref.shape[0]
    place = lax.broadcasted_iota(jnp.int32, (rows, LANES), 1) // slots
    for q, row in enumerate(wanted_rows):
        wanted = jnp.broadcast_to(row, (rows, LANES))
        acc = jnp.zeros((rows, LANES), jnp.float32)
        for j in range(per):
            start = (q * per + j) * LANES
            block = ref[:, start : start + LANES].astype(jnp.float32)
            taken = jnp.take_along_axis(block, wanted, axis=1, mode="promise_in_bounds")
            acc = jnp.where(place == j, taken, acc)
        yield q, acc


def gather_kernel(slots, groups, skip, base_ref, index_ref, *refs):
    out_ref = refs[-1]
    lines = out_ref.shape[2] // LANES
    first = (skip + pl.program_id(0)) * lines
    for i, group in enumerate(groups):
        rows = [index_ref[group, pl.ds(first + q, 1), :] for q in range(lines)]
        for q, taken in take_rows(slots, refs[i], rows):
            out_ref[i, :, q * LANES : (q + 1) * LANES] = taken.astype(out_ref.dtype)


def gather(states, groups, index, base, slots, piece, eighth=0):
    rows = states[0].shape[0]
    width = piece // 8
    steps = 8 - eighth
    observations = width // LANES * slots * steps
    state_spec = pl.BlockSpec((rows, width), lambda i, base: (0, base[0] * 8 + eighth + i))
    return pl.pallas_call(
        functools.partial(gather_kernel, slots, groups, eighth),
        out_shape=jax.ShapeDtypeStruct((len(groups), rows, observations), jnp.bfloat16),
        grid_spec=pltpu.PrefetchScalarGridSpec(
            num_scalar_prefetch=1,
            grid=(steps,),
            in_specs=[pl.BlockSpec(index.shape, lambda i, base: (0, 0, 0))]
            + [state_spec] * len(groups),
            out_specs=pl.BlockSpec(
                (len(groups), rows, observations // steps), lambda i, base: (0, 0, i)
            ),
        ),
        compiler_params=pltpu.CompilerParams(dimension_semantics=("arbitrary",), vmem_limit_bytes=VMEM),
        name="gather",
    )(base, index, *[states[group] for group in groups])


def add_statistics(hx, value, wt, live, total_ref, so_far_ref):
    everyone = hx.shape[0]
    hmean = jnp.sum(hx, axis=0, keepdims=True) / everyone
    anomaly = hx - hmean
    innov = value - hmean
    scaled = anomaly * wt
    product = lax.dot_general(
        jnp.concatenate(split(scaled), axis=0),
        jnp.concatenate(split(anomaly), axis=0),
        (((1,), (1,)), ((), ())),
        preferred_element_type=jnp.float32,
    )

    def term(i, j):
        rows = product[i * everyone : (i + 1) * everyone]
        return rows[:, j * everyone : (j + 1) * everyone]

    gram = term(0, 0) + (term(0, 1) + term(1, 0) + (term(0, 2) + term(2, 0) + term(1, 1)))
    cross = jnp.sum(scaled * innov, axis=1, keepdims=True)
    misfit = jnp.sum(wt * innov * innov, axis=1, keepdims=True)
    count = jnp.sum(live, axis=1, keepdims=True)
    lane = lax.broadcasted_iota(jnp.int32, (everyone, LANES - everyone), 1)
    side = jnp.where(lane == 0, cross, jnp.where(lane == 1, misfit, jnp.where(lane == 2, count, 0.0)))
    new = jnp.concatenate([gram, side], axis=1)

    @pl.when(pl.program_id(0) == 0)
    def _():
        total_ref[...] = new if so_far_ref is None else so_far_ref[...] + new

    @pl.when(pl.program_id(0) > 0)
    def _():
        total_ref[...] += new


def statistics_kernel(parts, slots, group, first, lines, started, me_ref, *refs):
    part_refs = refs[:parts]
    refs = refs[parts:]
    value_ref, weight_ref, live_ref = refs[:3]
    refs = refs[3:]
    index_ref = None
    if lines:
        index_ref, *refs = refs
    so_far_ref = None
    if started:
        so_far_ref, *refs = refs
    total_ref, all_ref = refs
    members = part_refs[0].shape[-2]
    me = me_ref[0]

    def place(j):
        return pl.ds(pl.multiple_of(lax.rem(me + j, parts) * members, members), members)

    all_ref[place(0), :] = part_refs[0][0].astype(jnp.float32)
    for j in range(1, parts):
        if not lines:
            all_ref[place(j), :] = part_refs[j][0].astype(jnp.float32)
            continue
        at = first + pl.program_id(0) * lines
        rows = [index_ref[group, pl.ds(at + q, 1), :] for q in range(lines)]
        for q, taken in take_rows(slots, part_refs[j], rows):
            all_ref[place(j), q * LANES : (q + 1) * LANES] = taken
    add_statistics(
        all_ref[...], value_ref[0], weight_ref[0], live_ref[0], total_ref, so_far_ref
    )


def statistics(own, others, value, weight, live, me, group, lo, hi, so_far, index=None, slots=0):
    members = own.shape[1]
    parts = 1 + len(others)
    everyone = members * parts
    if index is None:
        width = math.gcd(math.gcd(lo, hi), 1024)
        lines = 0
        other_spec = pl.BlockSpec((1, members, width), lambda i, me: (0, 0, i))
    else:
        width = math.gcd(math.gcd(lo, hi), 512)
        lines = width // LANES
        other_spec = pl.BlockSpec(
            (members, width // slots * LANES), lambda i, me: (0, i)
        )
    skip = lo // width
    in_specs = [pl.BlockSpec((1, members, width), lambda i, me: (group, 0, skip + i))]
    in_specs += [other_spec] * len(others)
    in_specs += [pl.BlockSpec((1, 1, width), lambda i, me: (group, 0, skip + i))] * 3
    operands = [own, *others, value, weight, live]
    if index is not None:
        in_specs.append(pl.BlockSpec(index.shape, lambda i, me: (0, 0, 0)))
        operands.append(index)
    if so_far is not None:
        in_specs.append(pl.BlockSpec((everyone, LANES), lambda i, me: (0, 0)))
        operands.append(so_far)
    return pl.pallas_call(
        functools.partial(
            statistics_kernel, parts, slots, group, lo // LANES, lines, so_far is not None
        ),
        out_shape=jax.ShapeDtypeStruct((everyone, LANES), jnp.float32),
        grid_spec=pltpu.PrefetchScalarGridSpec(
            num_scalar_prefetch=1,
            grid=((hi - lo) // width,),
            in_specs=in_specs,
            out_specs=pl.BlockSpec((everyone, LANES), lambda i, me: (0, 0)),
            scratch_shapes=[pltpu.VMEM((everyone, width), jnp.float32)],
        ),
        compiler_params=pltpu.CompilerParams(dimension_semantics=("arbitrary",), vmem_limit_bytes=VMEM),
        name="statistics",
    )(me, *operands)


def transform_kernel(members, me_ref, stats_ref, transform_ref, mixer_ref, rest_ref):
    stats = stats_ref[...]
    everyone = stats.shape[0]
    gram = stats[:, :everyone]
    cross = stats[:, everyone : everyone + 1]
    misfit = stats[0:1, everyone + 1 : everyone + 2]
    total = stats[0:1, everyone + 2 : everyone + 3]
    dof = everyone - 1.0
    row = lax.broadcasted_iota(jnp.int32, (everyone, everyone), 0)
    col = lax.broadcasted_iota(jnp.int32, (everyone, everyone), 1)
    eye = (row == col).astype(jnp.float32)
    scl = dof / total
    gs = scl * gram
    bs = scl * cross
    qval = scl * misfit

    def whole_sum(x):
        return jnp.sum(jnp.sum(x, axis=1, keepdims=True), axis=0, keepdims=True)

    tval = whole_sum(gs * eye)
    rho = (1.0 + qval / dof) / (1.0 + tval / dof)
    amat = dof / rho * eye + gs
    scale = jnp.sqrt(whole_sum(amat * amat))

    def forward_step(_, carry):
        yn, zn = (split(x) for x in carry)
        tm = split(1.5 * eye - 0.5 * terms_dot(zn, yn))
        return terms_dot(yn, tm), terms_dot(tm, zn)

    yn = amat / scale
    tm = 1.5 * eye - 0.5 * yn
    yn, zn = lax.fori_loop(1, ITERS, forward_step, (terms_dot(split(yn), split(tm)), tm))
    parts = split(zn)
    pmat = terms_dot(parts, parts) / scale
    wide = jnp.broadcast_to(bs, (everyone, LANES))
    wbar = terms_dot(split(pmat), split(wide))[:, 0:1]
    transform = jnp.sqrt(dof) * zn / jnp.sqrt(scale) + wbar
    transform_ref[...] = transform
    held = pltpu.roll(transform, lax.rem(everyone - me_ref[0] * members, everyone), 0)
    mixer = held.T.astype(jnp.bfloat16)
    column_total = jnp.sum(mixer.astype(jnp.float32), axis=1, keepdims=True)
    extra = mixer_ref.shape[0] - everyone
    mixer_ref[...] = jnp.concatenate([mixer, jnp.ones((extra, everyone), jnp.bfloat16)], axis=0)
    rest_ref[...] = jnp.broadcast_to((1.0 - column_total) / everyone, rest_ref.shape)


def make_transform(stats, members, me):
    everyone = stats.shape[0]
    return pl.pallas_call(
        functools.partial(transform_kernel, members),
        out_shape=(
            jax.ShapeDtypeStruct((everyone, everyone), jnp.float32),
            jax.ShapeDtypeStruct((everyone + 16, everyone), jnp.bfloat16),
            jax.ShapeDtypeStruct((everyone, LANES), jnp.float32),
        ),
        in_specs=[pl.BlockSpec(memory_space=pltpu.SMEM), pl.BlockSpec(memory_space=pltpu.VMEM)],
        out_specs=(pl.BlockSpec(memory_space=pltpu.VMEM),) * 3,
        compiler_params=pltpu.CompilerParams(vmem_limit_bytes=VMEM),
        name="transform",
    )(me, stats)


def step_pieces(bounds, start, end):
    pieces = []
    for i, (lo, hi) in enumerate(bounds):
        if lo < end and start < hi:
            pieces.append((i, max(lo, start) - lo, min(hi, end) - lo))
    return pieces


def analysis_kernel(bounds, sources, skip, aliased, base_ref, mixer_ref, rest_ref, own_ref, *refs):
    out_ref = refs[len(bounds) * sources + aliased]
    everyone, width = out_ref.shape
    members = own_ref.shape[0]
    rest = rest_ref[:, 0:1]
    for step in range((bounds[-1][1] - bounds[0][0]) // width):

        @pl.when(pl.program_id(0) == step)
        def _(step=step):
            start = (skip + step) * width
            pieces = step_pieces(bounds, start, start + width)
            cols = [own_ref[...]]
            for source in range(sources):
                parts = [refs[i * sources + source][:, lo:hi] for i, lo, hi in pieces]
                cols.append(parts[0] if len(parts) == 1 else jnp.concatenate(parts, axis=1))
            if members % 16:
                cols = [x.astype(jnp.float32) for x in cols]
            cols = jnp.concatenate(cols, axis=0).astype(jnp.bfloat16)
            mixed = jnp.dot(mixer_ref[...], cols, preferred_element_type=jnp.float32)
            out = mixed[:everyone] + rest * mixed[everyone : everyone + 1]
            out_ref[...] = out.astype(out_ref.dtype)


def analyse(out, state, messages, mixer, rest, base, piece):
    members = state.shape[0]
    everyone = rest.shape[0]
    bounds = tuple((lo, hi) for lo, hi, _ in messages)
    first, last = bounds[0][0], bounds[-1][1]
    width = math.gcd(piece // 4, first, last)
    skip = first // width
    whole = piece // width
    received = [x for _, _, pieces in messages for x in pieces]
    aliased = int(out is not None)
    in_specs = [
        pl.BlockSpec(mixer.shape, lambda i, base: (0, 0)),
        pl.BlockSpec(rest.shape, lambda i, base: (0, 0)),
        pl.BlockSpec((members, width), lambda i, base: (0, base[0] * whole + skip + i)),
    ] + [pl.BlockSpec(memory_space=pltpu.VMEM)] * len(received)
    operands = [base, mixer, rest, state, *received]
    aliases = {}
    if aliased:
        in_specs.append(pl.BlockSpec(memory_space=pl.ANY))
        aliases = {len(operands): 0}
        operands.append(out)
    return pl.pallas_call(
        functools.partial(
            analysis_kernel, bounds, len(received) // len(messages), skip, aliased
        ),
        out_shape=jax.ShapeDtypeStruct((everyone, piece), jnp.bfloat16),
        grid_spec=pltpu.PrefetchScalarGridSpec(
            num_scalar_prefetch=1,
            grid=((last - first) // width,),
            in_specs=in_specs,
            out_specs=pl.BlockSpec((everyone, width), lambda i, base: (0, skip + i)),
        ),
        input_output_aliases=aliases,
        compiler_params=pltpu.CompilerParams(
            dimension_semantics=("arbitrary",), vmem_limit_bytes=VMEM
        ),
        name="analysis",
    )(*operands)


def shards(state_a, state_b, obs_index, observation_count, obs_value, obs_weight):
    states = (state_a, state_b)
    members = state_a.shape[0]
    nmem = lax.axis_size("mem")
    ncol = lax.axis_size("col")
    piece = state_a.shape[1] // nmem
    nblk = obs_index.shape[1]
    slots = obs_index.shape[2]
    observations = nblk * slots
    unit = piece // 32
    me = lax.axis_index("mem")
    me_ref = me[None].astype(jnp.int32)
    shifts = range(1, nmem)

    def to_lower(array, shift):
        return lax.ppermute(array, "mem", [(i, (i - shift) % nmem) for i in range(nmem)])

    def to_upper(array, shift):
        return lax.ppermute(array, "mem", [(i, (i + shift) % nmem) for i in range(nmem)])

    def cut(message, source):
        group, lo, hi = message
        return [
            lax.dynamic_slice(
                source[group],
                (0, lax.rem(me + nmem - shift, nmem) * piece + lo * unit),
                (members, (hi - lo) * unit),
            )
            for shift in shifts
        ]

    others_index = [to_upper(obs_index, shift) for shift in shifts]
    index, *others_index = (
        x.reshape(2, observations // LANES, LANES) for x in (obs_index, *others_index)
    )

    group, lo, hi = MESSAGES[0]
    first_pieces = [
        cut_out(
            states[group],
            lax.rem(me_ref + nmem - shift, nmem),
            lo * unit,
            hi * unit,
            piece,
            MOST_VMEM,
        )
        for shift in shifts
    ]
    own_hx = gather(states, (0, 1), index, me_ref, slots, piece)
    sent_hx = [
        gather(states, SENT[:1], idx, lax.rem(me_ref + nmem - shift, nmem), slots, piece, SENT[1])
        for idx, shift in zip(others_index, shifts)
    ]
    got_hx = [to_lower(x, shift) for x, shift in zip(sent_hx, shifts)]

    live = (
        lax.broadcasted_iota(jnp.int32, (2, nblk, slots), 2) < observation_count[:, :, None]
    ).astype(jnp.float32)
    weight = (live * obs_weight).reshape(2, 1, observations)
    live = live.reshape(2, 1, observations)
    value = obs_value.reshape(2, 1, observations)

    received = {}

    def send(i, pieces):
        received[i] = [to_lower(x, shift) for x, shift in zip(pieces, shifts)]

    send(0, first_pieces)
    sources = lax.optimization_barrier((*states, sent_hx))
    for i, message in enumerate(MESSAGES[1:-1], 1):
        pieces = cut(message, sources)
        send(i, pieces)

    def read(i, so_far):
        group, lo, hi = MESSAGES[i]
        lo, hi = (x * observations // 32 for x in (lo, hi))
        return statistics(
            own_hx, received[i], value, weight, live, me_ref, group, lo, hi, so_far, index, slots
        )

    stats = read(READ[0], None)
    stats = statistics(
        own_hx,
        got_hx,
        value,
        weight,
        live,
        me_ref,
        SENT[0],
        SENT[1] * observations // 8,
        observations,
        stats,
    )
    for i in READ[1:]:
        stats = read(i, stats)

    group, lo, hi = MESSAGES[-1]
    source = lax.optimization_barrier((states[group], stats))[0]
    pieces = [
        cut_out(source, lax.rem(me_ref + nmem - shift, nmem), lo * unit, hi * unit, piece, VMEM)
        for shift in shifts
    ]
    send(len(MESSAGES) - 1, pieces)

    def all_sum(x, axis, size):
        for i in range((size - 1).bit_length()):
            x = x + lax.ppermute(x, axis, [(j, j ^ (1 << i)) for j in range(size)])
        return x

    stats = all_sum(all_sum(stats, "mem", nmem), "col", ncol)
    transform, mixer, rest = make_transform(stats, members, me_ref)

    outs = [None, None]
    for call in CALLS:
        group = MESSAGES[call[0]][0]
        messages = [
            (MESSAGES[m][1] * unit, MESSAGES[m][2] * unit, received[m]) for m in call
        ]
        outs[group] = analyse(
            outs[group], states[group], messages, mixer, rest, me_ref, piece
        )
    return (outs[0], outs[1], transform)


def solution(mesh):
    return jax.shard_map(
        shards,
        mesh=mesh,
        in_specs=(
            P("mem", "col"),
            P("mem", "col"),
            P(None, ("col", "mem"), None),
            P(None, ("col", "mem")),
            P(None, ("col", "mem"), None),
            P(None, ("col", "mem"), None),
        ),
        out_specs=(P(None, ("col", "mem")), P(None, ("col", "mem")), P()),
        check_vma=False,
    )
```
